256 devices in a mesh: row: 8 (over y, core), col: 32 (over x, z).
Axes of the slice: x: 4, y: 4, z: 8, core: 2. Of those that a mesh axis runs over, the one named last changes fastest.
Arguments:
- matrix: float32 [4096, 4096], P('row', 'col'), may hold values from -12 to 12, as said below
Outputs:
- sign_estimate: float32 [4096, 4096], P('row', 'col')
The draws below stay inside these ranges and needn't reach their ends.
Inputs may be any that keep to these rules, and one draw needn't show every extreme that they name: `matrix`: symmetric; the magnitudes of its eigenvalues, divided by the root mean square of all its eigenvalues, lie between 0.4 and 1.7.
All inputs are finite; a program needn't handle non-finite values.
Results may differ from the reference program's by a relative error of at most 0.0002.
Values sent between devices are 32-bit elements; how exact they have to be, the bound alone decides.
A program may use at most 64 MiB of HBM per device.

```python
import math
import jax
import jax.numpy as jnp
from jax import lax

N = 4096
ITERS = 2


def draw_matrix(key, part):
    keys = jax.random.split(jax.random.fold_in(key, 23), 4)
    mixing = 1.0
    factor_low = 0.9
    factor_high = 1.1
    scale_low = 0.25
    scale_high = 4.0
    rough = jax.random.normal(keys[0], (N, N), jnp.float32) * (mixing / math.sqrt(N))
    basis, upper = jnp.linalg.qr(jnp.eye(N, dtype=jnp.float32) + rough)
    place = jnp.arange(N, dtype=jnp.float32) / N
    factor = jax.random.uniform(keys[1], (N,), jnp.float32, factor_low, factor_high)
    signs = jax.random.rademacher(keys[2], (N,), jnp.float32)
    overall = jnp.exp(jax.random.uniform(keys[3], (), jnp.float32, math.log(scale_low), math.log(scale_high)))
    spectrum = signs * (0.6 + 0.9 * place) * factor * overall
    product = jnp.dot(basis * spectrum[None, :], basis.T, precision=lax.Precision.HIGHEST)
    return 0.5 * (product + product.T)


def setup_inputs(seed: int = 0) -> dict:
    arg_keys = jax.random.split(jax.random.key(seed), 2)
    matrix = draw_matrix(jax.random.fold_in(arg_keys[1], 71), 0)
    return dict(matrix=matrix)


def reference(matrix):
    total = jnp.sum(matrix * matrix)
    x_iter = matrix * jnp.sqrt(N / total)
    for step in range(ITERS):
        square = jnp.dot(x_iter.astype(jnp.float32), x_iter.astype(jnp.float32), preferred_element_type=jnp.float32, precision=lax.Precision.HIGHEST)
        cube_block = jnp.dot(x_iter.astype(jnp.float32), square.astype(jnp.float32), preferred_element_type=jnp.float32, precision=lax.Precision.HIGHEST)
        x_iter = 1.5 * x_iter - 0.5 * cube_block
    return x_iter
```

```python
import functools

import jax
import jax.numpy as jnp
from jax import lax
from jax.experimental import pallas as pl
from jax.experimental.pallas import tpu as pltpu
from jax.sharding import Mesh
from jax.sharding import PartitionSpec as P

N = 4096
ITERS = 2
NY, NC, NX, NZ = 4, 2, 4, 8
ROWS = N // (NY * NC)
STRIP = N // (NX * NZ)
HALF = ROWS // 2
QROWS = STRIP // (2 * NY)
GROUPS = ((0, 3), (3, 2), (5, 2), (7, 1))
BF = jnp.bfloat16
F32 = jnp.float32


def split(value):
    high = value.astype(BF)
    return high, (value - high.astype(F32)).astype(BF)


def three(dot, a, b):
    return dot(a[0], b[0]) + (dot(a[0], b[1]) + dot(a[1], b[0]))


def dot_nn(a, b):
    return lax.dot_general(a, b, (((1,), (0,)), ((), ())), preferred_element_type=F32)


def dot_tn(a, b):
    return lax.dot_general(a, b, (((0,), (0,)), ((), ())), preferred_element_type=F32)


def kernel(
    m_ref, o_ref,
    block, panel, block_hi, block_lo, panel_hi, panel_lo,
    part, from_core, mine, chain, ended, square, cube, x_chain, x_ended, factor, sums_x, sums_y,
    z_send, z_recv, x_send, x_recv, g_send, g_recv, s_send, s_recv,
):
    y, c, x, z = (lax.axis_index(name) for name in ("y", "c", "x", "z"))

    def turn(name, here, by, size):
        return {name: lax.rem(here + by, size)}

    up_z, down_z = turn("z", z, 1, NZ), turn("z", z, NZ - 1, NZ)
    up_x, down_x = turn("x", x, 1, NX), turn("x", x, NX - 1, NX)
    up_y, down_y = turn("y", y, 1, NY), turn("y", y, NY - 1, NY)
    other_core = {"c": 1 - c}
    x_peers = [turn("x", x, d, NX) for d in range(1, NX)]
    y_peers = [{"y": lax.rem(y + d, NY), "c": lax.rem(c + e, NC)} for d in range(NY) for e in range(NC)][1:]

    barrier = pltpu.get_barrier_semaphore()
    peers = [up_z, down_z, *x_peers, *y_peers]
    for peer in peers:
        pl.semaphore_signal(barrier, inc=1, device_id=peer, device_id_type=pl.DeviceIdType.MESH)

    pending = []

    def copy(src, dst, send, recv, peer):
        return pltpu.make_async_remote_copy(
            src_ref=src, dst_ref=dst, send_sem=send, recv_sem=recv,
            device_id=peer, device_id_type=pl.DeviceIdType.MESH,
        )

    def go(made):
        made.start()
        pending.append(made)

    def quarter(by):
        return lax.rem(y + by, NY)

    for it in range(ITERS):
        block_i, panel_i = block.at[it], panel.at[it]

        def z_copy(src_pos, dst_pos, piece, peer):
            rows = pl.ds(piece * HALF, HALF)
            return copy(
                block_i.at[src_pos, rows], block_i.at[dst_pos, rows],
                z_send.at[it, dst_pos, piece], z_recv.at[it, dst_pos, piece], peer,
            )

        ups = {(p, q): z_copy({2: 0, 4: 2, 6: 4}[p], p, q, up_z) for p in (2, 4, 6) for q in (0, 1)}
        downs = {(p, q): z_copy({1: 0, 3: 1, 5: 3}[p], p, q, down_z) for p in (1, 3, 5) for q in (0, 1)}
        ups[7, 0] = z_copy(6, 7, 0, up_z)
        downs[7, 1] = z_copy(5, 7, 1, down_z)

        def x_copy(src, dst, piece, k, peer):
            rows = pl.ds(piece * HALF, HALF)
            return copy(src.at[rows], panel_i.at[dst, rows], x_send.at[it, k], x_recv.at[it, k], peer)

        own = block_i.at[0]
        x_up = [x_copy(own, 3, 0, 0, up_x), x_copy(own, 3, 1, 1, up_x)]
        x_down = [x_copy(own, 1, 0, 2, down_x), x_copy(own, 1, 1, 3, down_x)]
        x_up_far = x_copy(panel_i.at[3], 2, 0, 4, up_x)
        x_down_far = x_copy(panel_i.at[1], 2, 1, 5, down_x)

        def start_all():
            if it == 0:
                block_i[0] = m_ref[...]
                pl.semaphore_wait(barrier, len(peers))
            for q in (0, 1):
                go(x_up[q])
                go(x_down[1 - q])
                go(ups[2, q])
                go(downs[1, q])
            put_panel(0, block_i[0])
            put_block(0)

        def put_panel(slot, value):
            columns = slice(slot * STRIP, (slot + 1) * STRIP)
            panel_hi[:, columns], panel_lo[:, columns] = split(value)

        def put_block(pos):
            columns = slice(pos * STRIP, (pos + 1) * STRIP)
            block_hi[:, columns], block_lo[:, columns] = split(block_i[pos])

        def z_step(pos, piece):
            downs[pos, piece].wait_recv()
            if (pos + 2, piece) in downs:
                go(downs[pos + 2, piece])
            ups[pos + 1, piece].wait_recv()
            if (pos + 3, piece) in ups:
                go(ups[pos + 3, piece])
            if pos == 5 and piece == 0:
                go(ups[7, 0])
            if piece == 1:
                put_block(pos)
                put_block(pos + 1)

        def z_last():
            ups[7, 0].wait_recv()
            downs[7, 1].wait_recv()
            put_block(7)

        def x_far():
            x_up[0].wait_recv()
            go(x_up_far)
            x_down[1].wait_recv()
            go(x_down_far)

        def x_near():
            x_up[1].wait_recv()
            x_down[0].wait_recv()
            put_panel(3, panel_i[3])
            put_panel(1, panel_i[1])

        def x_last():
            x_up_far.wait_recv()
            x_down_far.wait_recv()
            put_panel(2, panel_i[2])

        def group_copies(g):
            first, n = GROUPS[g]
            run = pl.ds(first, n)

            def made(k, src, dst, peer):
                return copy(src, dst, g_send.at[it, g, k], g_recv.at[it, g, k], peer)

            low, high = pl.ds(0, QROWS // 2), pl.ds(QROWS // 2, QROWS // 2)
            w, r1, r2, s = mine.at[it, run], chain.at[it, run], ended.at[it, run], square.at[it, run]
            at = lambda ref, *where: ref.at[(slice(None), *where)]
            return dict(
                core=made(0, at(part.at[it, run], 1 - c), from_core.at[it, run], other_core),
                chain_up=made(1, at(w, quarter(2), low), at(r1, 0), up_y),
                chain_down=made(2, at(w, quarter(2), high), at(r1, 1), down_y),
                near_down=made(3, at(w, quarter(3), low), at(r1, 2), down_y),
                near_up=made(4, at(w, quarter(1), high), at(r1, 3), up_y),
                end_up=made(5, at(w, quarter(1), low), at(r2, 0), up_y),
                end_down=made(6, at(w, quarter(3), high), at(r2, 1), down_y),
                give_up=made(7, at(s, c, y), at(s, c, y), up_y),
                give_down=made(8, at(s, c, y), at(s, c, y), down_y),
                far_up=made(9, at(s, c, quarter(3), low), at(s, c, quarter(3), low), up_y),
                far_down=made(10, at(s, c, quarter(1), high), at(s, c, quarter(1), high), down_y),
                join=made(11, at(s, c), at(s, c), other_core),
            )

        def multiply(g, cs):
            first, n = GROUPS[g]
            columns = slice(first * STRIP, (first + n) * STRIP)
            a = block_hi[:, columns], block_lo[:, columns]
            got = three(dot_tn, a, (panel_hi[...], panel_lo[...]))
            part[it, first : first + n] = got.reshape(n, NC, NY * QROWS, NX * STRIP)
            go(cs["core"])

        def step1(g, cs):
            first, n = GROUPS[g]
            cs["core"].wait_recv()
            for p in range(first, first + n):
                total = part[it, p, c] + from_core[it, p]
                mine[it, p] = total.reshape(NY, QROWS, NX * STRIP)
            for name in ("chain_up", "chain_down", "near_up", "near_down"):
                go(cs[name])

        def step2(g, cs):
            first, n = GROUPS[g]
            h = QROWS // 2
            cs["chain_up"].wait_recv()
            for p in range(first, first + n):
                mine[it, p, quarter(1), 0:h] += chain[it, p, 0]
            go(cs["end_up"])
            cs["chain_down"].wait_recv()
            for p in range(first, first + n):
                mine[it, p, quarter(3), h : 2 * h] += chain[it, p, 1]
            go(cs["end_down"])

        def step3(g, cs):
            first, n = GROUPS[g]
            h = QROWS // 2
            for name in ("near_down", "near_up", "end_up", "end_down"):
                cs[name].wait_recv()
            for p in range(first, first + n):
                square[it, p, c, y, 0:h] = mine[it, p, y, 0:h] + (ended[it, p, 0] + chain[it, p, 2])
                square[it, p, c, y, h : 2 * h] = mine[it, p, y, h : 2 * h] + (ended[it, p, 1] + chain[it, p, 3])
            go(cs["give_up"])
            go(cs["give_down"])

        def step4(g, cs):
            cs["give_up"].wait_recv()
            go(cs["far_up"])
            cs["give_down"].wait_recv()
            go(cs["far_down"])

        def step5(g, cs):
            cs["far_up"].wait_recv()
            cs["far_down"].wait_recv()
            go(cs["join"])

        def step6(g, cs):
            first, n = GROUPS[g]
            cs["join"].wait_recv()
            value = square[it, first : first + n].reshape(n * STRIP, NX * STRIP)
            if it == 0:
                f = factor[0:1, 0:1]
                value = value * (f * f)
            columns = slice(first * STRIP, (first + n) * STRIP)
            a = block_hi[:, columns], block_lo[:, columns]
            got = three(dot_nn, a, split(value))
            for d in range(NX):
                piece = got[:, d * STRIP : (d + 1) * STRIP]
                if g == 0:
                    cube[it, d] = piece
                else:
                    cube[it, d] += piece

        def sums1():
            tile = jnp.zeros((8, 128), F32)
            for p in range(NZ):
                v = block_i[p].reshape(ROWS // 8, 8, STRIP)
                tile = tile + jnp.sum(v * v, axis=0)
            sums_x[0] = tile
            for k in range(1, NX):
                go(sx[k])

        def sums2():
            for k in range(1, NX):
                sx[k].wait_recv()
            sums_y[0] = (sums_x[0] + sums_x[1]) + (sums_x[2] + sums_x[3])
            for k in range(1, NY * NC):
                go(sy[k])

        def sums3():
            for k in range(1, NY * NC):
                sy[k].wait_recv()
            total = jnp.sum(jnp.sum(sums_y[...], axis=0), keepdims=True)
            factor[...] = jnp.broadcast_to(jnp.sqrt(N / total), factor.shape)

        sx = {k: copy(sums_x.at[0], sums_x.at[k], s_send.at[k], s_recv.at[k], x_peers[k - 1])
            for k in (range(1, NX) if it == 0 else ())}
        sy = {
            k: copy(sums_y.at[0], sums_y.at[k], s_send.at[NX + k], s_recv.at[NX + k], y_peers[k - 1])
            for k in (range(1, NY * NC) if it == 0 else ())
        }

        cs = [group_copies(g) for g in range(len(GROUPS))]
        low, high = pl.ds(0, HALF), pl.ds(HALF, HALF)

        def r_copy(k, src, dst, peer):
            return copy(src, dst, x_send.at[it, 6 + k], x_recv.at[it, 6 + k], peer)

        cb = cube.at[it]
        r_chain_up = r_copy(0, cb.at[2, low], x_chain.at[it, 0], up_x)
        r_chain_down = r_copy(1, cb.at[2, high], x_chain.at[it, 1], down_x)
        r_near_down = r_copy(2, cb.at[3, low], x_chain.at[it, 2], down_x)
        r_near_up = r_copy(3, cb.at[1, high], x_chain.at[it, 3], up_x)
        r_end_up = r_copy(4, cb.at[1, low], x_ended.at[it, 0], up_x)
        r_end_down = r_copy(5, cb.at[3, high], x_ended.at[it, 1], down_x)

        def finish():
            go(r_chain_up)
            go(r_chain_down)
            go(r_near_down)
            go(r_near_up)
            r_chain_up.wait_recv()
            cube[it, 1, 0:HALF] += x_chain[it, 0]
            go(r_end_up)
            r_chain_down.wait_recv()
            cube[it, 3, HALF:ROWS] += x_chain[it, 1]
            go(r_end_down)
            r_near_down.wait_recv()
            r_near_up.wait_recv()
            for k, (end, rows) in enumerate(((r_end_up, slice(0, HALF)), (r_end_down, slice(HALF, ROWS)))):
                end.wait_recv()
                product = cube[it, 0, rows] + (x_ended[it, k] + x_chain[it, 2 + k])
                value = block_i[0, rows]
                if it == 0:
                    f = factor[0:1, 0:1]
                    new = (1.5 * f) * value - (0.5 * f) * product
                else:
                    new = 1.5 * value - 0.5 * product
                if it == ITERS - 1:
                    o_ref[rows] = new
                else:
                    block[it + 1, 0, rows] = new

        events = [
            (0.0, start_all),
            (4.5, functools.partial(z_step, 1, 0)),
            (4.6, x_far),
            (7.2, functools.partial(z_step, 1, 1)),
            (7.3, x_near),
            (10.0, functools.partial(z_step, 3, 0)),
            (10.1, x_last),
            (12.9, functools.partial(z_step, 3, 1)),
            (15.7, functools.partial(z_step, 5, 0)),
            (18.5, functools.partial(z_step, 5, 1)),
            (21.3, z_last),
        ]
        stages = (multiply, step1, step2, step3, step4, step5, step6)
        times = (
            (10.5, 13.0, 16.9, 19.8, 23.0, 26.0, 27.5),
            (12.95, 14.8, 18.4, 20.6, 24.0, 27.0, 28.6),
            (18.6, 20.4, 22.6, 25.0, 27.2, 29.2, 30.8),
            (21.4, 23.5, 25.5, 28.0, 30.0, 32.0, 33.5),
        )
        for g in range(len(GROUPS)):
            for stage, when in zip(stages, times[g]):
                events.append((when, functools.partial(stage, g, cs[g])))
        if it == 0:
            events += [(21.5, sums1), (24.1, sums2), (27.1, sums3)]
        events.append((40.0, finish))
        for _, do in sorted(events, key=lambda e: e[0]):
            do()

    for made in pending:
        made.wait_send()


def shards(matrix):
    dma = pltpu.SemaphoreType.DMA
    wide = NX * STRIP
    return pl.pallas_call(
        kernel,
        out_shape=jax.ShapeDtypeStruct((ROWS, STRIP), F32),
        in_specs=[pl.BlockSpec(memory_space=pltpu.VMEM)],
        out_specs=pl.BlockSpec(memory_space=pltpu.VMEM),
        scratch_shapes=[
            pltpu.VMEM((ITERS, NZ, ROWS, STRIP), F32),
            pltpu.VMEM((ITERS, NX, ROWS, STRIP), F32),
            pltpu.VMEM((ROWS, NZ * STRIP), BF),
            pltpu.VMEM((ROWS, NZ * STRIP), BF),
            pltpu.VMEM((ROWS, wide), BF),
            pltpu.VMEM((ROWS, wide), BF),
            pltpu.VMEM((ITERS, NZ, NC, STRIP // 2, wide), F32),
            pltpu.VMEM((ITERS, NZ, STRIP // 2, wide), F32),
            pltpu.VMEM((ITERS, NZ, NY, QROWS, wide), F32),
            pltpu.VMEM((ITERS, NZ, 4, QROWS // 2, wide), F32),
            pltpu.VMEM((ITERS, NZ, 2, QROWS // 2, wide), F32),
            pltpu.VMEM((ITERS, NZ, NC, NY, QROWS, wide), F32),
            pltpu.VMEM((ITERS, NX, ROWS, STRIP), F32),
            pltpu.VMEM((ITERS, 4, HALF, STRIP), F32),
            pltpu.VMEM((ITERS, 2, HALF, STRIP), F32),
            pltpu.VMEM((8, 128), F32),
            pltpu.VMEM((NX, 8, 128), F32),
            pltpu.VMEM((NY * NC, 8, 128), F32),
            dma((ITERS, NZ, 2)),
            dma((ITERS, NZ, 2)),
            dma((ITERS, 12)),
            dma((ITERS, 12)),
            dma((ITERS, len(GROUPS), 12)),
            dma((ITERS, len(GROUPS), 12)),
            dma((NX + NY * NC,)),
            dma((NX + NY * NC,)),
        ],
        compiler_params=pltpu.CompilerParams(
            collective_id=0, has_side_effects=True, vmem_limit_bytes=56 * 1024 * 1024
        ),
    )(matrix)


def solution(mesh):
    grid = Mesh(mesh.devices.reshape(NY, NC, NX, NZ), ("y", "c", "x", "z"))
    spec = P(("y", "c"), ("x", "z"))
    return jax.shard_map(shards, mesh=grid, in_specs=(spec,), out_specs=spec, check_vma=False)
```

```python
import jax
import jax.numpy as jnp
from jax import lax
from jax.experimental import pallas as pl
from jax.experimental.pallas import tpu as pltpu
from jax.sharding import Mesh
from jax.sharding import PartitionSpec as P

N = 4096
ITERS = 2
NY, NC, NX, NZ = 4, 2, 4, 8
ROWS = N // (NY * NC)
STRIP = N // (NX * NZ)
HALF = ROWS // 2
SROWS = STRIP // NC
SHALF = SROWS // 2
GROUPS = ((0, 1), (1, 2), (3, 2), (5, 2), (7, 1))
SETS = ((2,), (1, 3), (0,))
LANES = ((0, 1), (1, 2), (3, 1))
BF = jnp.bfloat16
F32 = jnp.float32
ORDER = (
    (
        ("own",), ("put", 0), ("mul", 0, 2), ("s1", 0, 2), ("s2", 0, 2), ("zd", 1, 1, 0), ("zu", 2, 0, 0), ("xfu",),
        ("xfd",), ("s3", 0, 2), ("zu", 2, 1, 0), ("zd", 1, 0, 0), ("put", 2), ("put", 1), ("mul", 1, 2), ("xnear",),
        ("mul", 1, 1), ("mul", 0, 1), ("s1", 1, 2), ("s1", 1, 1), ("s1", 0, 1), ("zd", 3, 1, 0), ("zu", 4, 0, 0),
        ("xlast",), ("mul", 1, 0), ("sums1",), ("mul", 0, 0), ("s1", 1, 0), ("s1", 0, 0), ("s2", 1, 2),
        ("zu", 4, 1, 0), ("put", 4), ("zd", 3, 0, 0), ("put", 3), ("mul", 2), ("s2", 1, 1), ("s2", 0, 1),
        ("sums2",), ("s1", 2, 0), ("s1", 2, 1), ("s1", 2, 2), ("s2", 1, 0), ("zu", 6, 0, 0), ("zd", 5, 1, 0),
        ("s2", 0, 0), ("s3", 1, 2), ("s3", 1, 1), ("zu", 6, 1, 0), ("zd", 5, 0, 0), ("put", 5), ("put", 6),
        ("mul", 3), ("s3", 0, 1), ("s2", 2, 0), ("s1", 3, 0), ("s1", 3, 1), ("s1", 3, 2), ("s2", 2, 1), ("sums3",),
        ("put", 7), ("mul", 4), ("s2", 2, 2), ("s3", 1, 0), ("s3", 0, 0), ("s1", 4, 0), ("s1", 4, 1), ("s3", 2, 0),
        ("s1", 4, 2), ("s6", 0), ("s2", 3, 0), ("s6", 1), ("s2", 3, 1), ("s6", 2, 0), ("s2", 3, 2), ("s3", 2, 1),
        ("s3", 2, 2), ("s2", 4, 0), ("s6", 2, 1), ("s2", 4, 1), ("s6", 2, 2), ("s2", 4, 2), ("s3", 3, 0),
        ("s6", 3, 0), ("s3", 3, 1), ("s3", 3, 2), ("s3", 4, 0), ("s3", 4, 1), ("s6", 3, 1), ("s6", 4, 0), ("rc",),
        ("s3", 4, 2), ("s6", 3, 2), ("s6", 4, 1), ("rn",), ("s6", 4, 2), ("re",), ("fin",),
    ),
    (
        ("own",), ("put", 0), ("mul", 0, 2), ("s1", 0, 2), ("s2", 0, 2), ("zu", 2, 0, 0), ("zd", 1, 1, 0), ("xfu",),
        ("xfd",), ("s3", 0, 2), ("zu", 2, 1, 0), ("put", 2), ("zd", 1, 0, 0), ("put", 1), ("mul", 1, 2), ("xnear",),
        ("mul", 1, 1), ("mul", 0, 1), ("s1", 1, 2), ("s1", 1, 1), ("s1", 0, 1), ("zd", 3, 1, 0), ("zu", 4, 0, 0),
        ("xlast",), ("mul", 0, 0), ("mul", 1, 0), ("s1", 0, 0), ("s1", 1, 0), ("s2", 1, 2), ("zu", 4, 1, 0),
        ("put", 4), ("zd", 3, 0, 0), ("put", 3), ("mul", 2), ("s2", 1, 1), ("s2", 0, 1), ("s1", 2, 0), ("s2", 0, 0),
        ("s1", 2, 1), ("s1", 2, 2), ("zu", 6, 0, 0), ("zd", 5, 1, 0), ("s2", 1, 0), ("s3", 1, 2), ("s3", 1, 1),
        ("zd", 5, 0, 0), ("put", 5), ("zu", 6, 1, 0), ("put", 6), ("mul", 3), ("s3", 0, 1), ("s2", 2, 0),
        ("s3", 0, 0), ("s1", 3, 0), ("s1", 3, 1), ("s1", 3, 2), ("s6", 0), ("s2", 2, 1), ("put", 7), ("mul", 4),
        ("s2", 2, 2), ("s3", 1, 0), ("s3", 2, 0), ("s1", 4, 0), ("s1", 4, 1), ("s1", 4, 2), ("s6", 1), ("s2", 3, 0),
        ("s6", 2, 0), ("s2", 3, 1), ("s2", 3, 2), ("s3", 2, 1), ("s3", 2, 2), ("s2", 4, 0), ("s6", 2, 1),
        ("s2", 4, 1), ("s6", 2, 2), ("s2", 4, 2), ("s3", 3, 0), ("s6", 3, 0), ("s3", 3, 1), ("s3", 3, 2),
        ("s3", 4, 0), ("s3", 4, 1), ("s6", 3, 1), ("s6", 4, 0), ("rc",), ("s3", 4, 2), ("s6", 3, 2), ("s6", 4, 1),
        ("rn",), ("s6", 4, 2), ("re",), ("fin",),
    ),
)


def split(value):
    high = value.astype(BF)
    return high, (value - high.astype(F32)).astype(BF)


def three(dim, a, b):
    a = jnp.concatenate([a[0], a[1], a[0]], axis=dim)
    b = jnp.concatenate([b[0], b[0], b[1]], axis=0)
    return lax.dot_general(a, b, (((dim,), (0,)), ((), ())), preferred_element_type=F32)


def lanes_of(s):
    first, n = LANES[s]
    return slice(first * STRIP, (first + n) * STRIP)


def kernel(m_ref, o_ref, block, panel, block_hi, block_lo, panel_hi, panel_lo, square_hi, square_lo, *refs):
    ns = len(SETS)
    part, from_core, mine, first_in, ours, second_in, square = (refs[k * ns : (k + 1) * ns] for k in range(7))
    (
        cube, x_chain, x_ended, factor, sums_y, sums_z,
        z_send, z_recv, x_send, x_recv, g_send, g_recv, s_send, s_recv,
    ) = refs[7 * ns :]
    y, c, x, z = (lax.axis_index(name) for name in ("y", "c", "x", "z"))

    def turn(name, here, by, size):
        return {name: lax.rem(here + by, size)}

    up_z, down_z = turn("z", z, 1, NZ), turn("z", z, NZ - 1, NZ)
    up_x, down_x = turn("x", x, 1, NX), turn("x", x, NX - 1, NX)
    odd = lax.rem(y, 2)
    y_near, y_far = turn("y", y, NY + 1 - 2 * odd, NY), turn("y", y, NY - 1 + 2 * odd, NY)
    other_core = {"c": 1 - c}
    z_peers = [turn("z", z, d, NZ) for d in range(1, NZ)]
    y_peers = [{"y": lax.rem(y + d, NY), "c": lax.rem(c + e, NC)} for d in range(NY) for e in range(NC)][1:]

    barrier = pltpu.get_barrier_semaphore()
    peers = [up_x, down_x, *z_peers, *y_peers]
    for peer in peers:
        pl.semaphore_signal(barrier, inc=1, device_id=peer, device_id_type=pl.DeviceIdType.MESH)
    block[0, 0] = m_ref[...]
    pl.semaphore_wait(barrier, len(peers))

    pending = []

    def copy(src, dst, send, recv, peer):
        return pltpu.make_async_remote_copy(
            src_ref=src, dst_ref=dst, send_sem=send, recv_sem=recv,
            device_id=peer, device_id_type=pl.DeviceIdType.MESH,
        )

    def go(made):
        made.start()
        pending.append(made)

    low, high = pl.ds(0, SHALF), pl.ds(SHALF, SHALF)

    def iteration(it):
        block_i, panel_i, cube_i = block.at[it], panel.at[it], cube.at[it]

        def z_copy(src, dst, piece, peer):
            rows = pl.ds(piece * HALF, HALF)
            return copy(
                block_i.at[src, rows], block_i.at[dst, rows],
                z_send.at[it, dst, piece], z_recv.at[it, dst, piece], peer,
            )

        ups = {(p, q): z_copy(max(p - 2, 0), p, q, up_z) for p in (2, 4, 6) for q in (0, 1)}
        downs = {(p, q): z_copy(max(p - 2, 0), p, q, down_z) for p in (1, 3, 5) for q in (0, 1)}
        ups[8, 0] = z_copy(6, 7, 0, up_z)
        downs[7, 1] = z_copy(5, 7, 1, down_z)

        def x_copy(src, dst, piece, k, peer):
            rows = pl.ds(piece * HALF, HALF)
            return copy(src.at[rows], panel_i.at[dst, rows], x_send.at[it, k], x_recv.at[it, k], peer)

        own_strip = block_i.at[0]
        x_up = [x_copy(own_strip, 3, 0, 0, up_x), x_copy(own_strip, 3, 1, 1, up_x)]
        x_down = [x_copy(own_strip, 1, 0, 2, down_x), x_copy(own_strip, 1, 1, 3, down_x)]
        x_up_far = x_copy(panel_i.at[3], 2, 0, 4, up_x)
        x_down_far = x_copy(panel_i.at[1], 2, 1, 5, down_x)

        def put_panel(slot, value):
            at = {2: 0, 1: 1, 3: 2, 0: 3}[slot]
            columns = slice(at * STRIP, (at + 1) * STRIP)
            panel_hi[:, columns], panel_lo[:, columns] = split(value)

        def own():
            for q in (0, 1):
                go(x_up[q])
                go(x_down[1 - q])
                go(ups[2, q])
                go(downs[1, 1 - q])

        def zd(pos, piece, _):
            downs[pos, piece].wait_recv()
            if (pos + 2, piece) in downs:
                go(downs[pos + 2, piece])

        def zu(pos, piece, _):
            ups[pos, piece].wait_recv()
            if (pos + 2, piece) in ups:
                go(ups[pos + 2, piece])

        def put(pos):
            if pos == 7:
                ups[8, 0].wait_recv()
                downs[7, 1].wait_recv()
            columns = slice(pos * STRIP, (pos + 1) * STRIP)
            value = block[it, pos]
            block_hi[:, columns], block_lo[:, columns] = split(value)
            if pos == 0:
                put_panel(0, value)

        def xfu():
            x_up[0].wait_recv()
            go(x_up_far)

        def xfd():
            x_down[1].wait_recv()
            go(x_down_far)

        def xnear():
            x_up[1].wait_recv()
            x_down[0].wait_recv()
            put_panel(3, panel[it, 3])
            put_panel(1, panel[it, 1])

        def xlast():
            x_up_far.wait_recv()
            x_down_far.wait_recv()
            put_panel(2, panel[it, 2])

        def unit(g, s):
            run = pl.ds(*GROUPS[g])
            every = slice(None)

            def made(k, src, dst, peer):
                return copy(src, dst, g_send.at[it, g, s, k], g_recv.at[it, g, s, k], peer)

            def rows(ref, which):
                return ref[s].at[it, run, which]

            sums = square[s].at[it, run, c]
            return dict(
                core=made(0, part[s].at[it, run, 1 - c], from_core[s].at[it, run], other_core),
                low_one=made(1, rows(mine, low), rows(first_in, low), y_near),
                high_one=made(2, rows(mine, high), rows(first_in, high), y_far),
                low_two=made(3, rows(ours, low), rows(second_in, low), y_far),
                high_two=made(4, rows(ours, high), rows(second_in, high), y_near),
                join=made(5, sums, sums, other_core),
            )

        units = {(g, s): unit(g, s) for g in range(len(GROUPS)) for s in range(ns)}

        def strips(g):
            first, n = GROUPS[g]
            return range(first, first + n)

        def factors(g):
            first, n = GROUPS[g]
            columns = slice(first * STRIP, (first + n) * STRIP)
            return block_hi[:, columns], block_lo[:, columns]

        def mul(g, *which):
            first, n = GROUPS[g]
            columns = lanes_of(which[0]) if which else slice(0, NX * STRIP)
            got = three(0, factors(g), (panel_hi[:, columns], panel_lo[:, columns]))
            for s in which or range(ns):
                piece = got if which else got[:, lanes_of(s)]
                part[s][it, first : first + n] = piece.reshape(n, NC, SROWS, piece.shape[1])
                go(units[g, s]["core"])

        def s1(g, s):
            cs = units[g, s]
            cs["core"].wait_recv()
            for p in strips(g):
                mine[s][it, p] = part[s][it, p, c] + from_core[s][it, p]
            go(cs["low_one"])
            go(cs["high_one"])

        def s2(g, s):
            cs = units[g, s]
            for one, two, rows in (("low_one", "low_two", low), ("high_one", "high_two", high)):
                cs[one].wait_recv()
                for p in strips(g):
                    ours[s][it, p, rows] = mine[s][it, p, rows] + first_in[s][it, p, rows]
                go(cs[two])

        def s3(g, s):
            cs = units[g, s]
            cs["low_two"].wait_recv()
            cs["high_two"].wait_recv()
            for p in strips(g):
                square[s][it, p, c] = ours[s][it, p] + second_in[s][it, p]
            go(cs["join"])

        def s6(g, *which):
            first, n = GROUPS[g]
            rows = slice(first * STRIP, (first + n) * STRIP)
            todo = which or range(ns)
            for s in todo:
                units[g, s]["join"].wait_recv()
                value = square[s][it, first : first + n]
                value = value.reshape(n * STRIP, value.shape[-1])
                if it == 0:
                    f = factor[0:1, 0:1]
                    value = value * (f * f)
                square_hi[rows, lanes_of(s)], square_lo[rows, lanes_of(s)] = split(value)
            columns = lanes_of(which[0]) if which else slice(0, NX * STRIP)
            got = three(1, factors(g), (square_hi[rows, columns], square_lo[rows, columns]))
            for k, slot in enumerate([slot for s in todo for slot in SETS[s]]):
                piece = got[:, k * STRIP : (k + 1) * STRIP]
                if first == 0:
                    cube[it, slot] = piece
                else:
                    cube[it, slot] += piece

        def r_copy(k, src, dst, peer):
            return copy(src, dst, x_send.at[it, 6 + k], x_recv.at[it, 6 + k], peer)

        upper, lower = slice(0, HALF), slice(HALF, ROWS)
        r_chain_up = r_copy(0, cube_i.at[2, upper], x_chain.at[it, 0], up_x)
        r_chain_down = r_copy(1, cube_i.at[2, lower], x_chain.at[it, 1], down_x)
        r_near_down = r_copy(2, cube_i.at[3, upper], x_chain.at[it, 2], down_x)
        r_near_up = r_copy(3, cube_i.at[1, lower], x_chain.at[it, 3], up_x)
        r_end_up = r_copy(4, cube_i.at[1, upper], x_ended.at[it, 0], up_x)
        r_end_down = r_copy(5, cube_i.at[3, lower], x_ended.at[it, 1], down_x)

        def rc():
            go(r_chain_up)
            go(r_chain_down)

        def rn():
            go(r_near_up)
            go(r_near_down)

        def re():
            r_chain_up.wait_recv()
            cube[it, 1, upper] += x_chain[it, 0]
            go(r_end_up)
            r_chain_down.wait_recv()
            cube[it, 3, lower] += x_chain[it, 1]
            go(r_end_down)

        def fin():
            r_near_down.wait_recv()
            r_near_up.wait_recv()
            for k, (end, rows) in enumerate(((r_end_up, upper), (r_end_down, lower))):
                end.wait_recv()
                product = cube[it, 0, rows] + (x_ended[it, k] + x_chain[it, 2 + k])
                value = block[it, 0, rows]
                if it == 0:
                    f = factor[0:1, 0:1]
                    new = (1.5 * f) * value - (0.5 * f) * product
                else:
                    new = 1.5 * value - 0.5 * product
                if it == ITERS - 1:
                    o_ref[rows] = new
                else:
                    block[it + 1, 0, rows] = new

        sy, sz = {}, {}
        if it == 0:
            for k, peer in enumerate(y_peers, 1):
                sy[k] = copy(sums_y.at[0], sums_y.at[k], s_send.at[k], s_recv.at[k], peer)
            for k, peer in enumerate(z_peers, 1):
                sz[k] = copy(sums_z.at[0], sums_z.at[k], s_send.at[8 + k], s_recv.at[8 + k], peer)

        def sums1():
            tile = jnp.zeros((8, 128), F32)
            for v in (block[it, 0], panel[it, 1], panel[it, 2], panel[it, 3]):
                v = v.reshape(ROWS // 8, 8, STRIP)
                tile = tile + jnp.sum(v * v, axis=0)
            sums_y[0] = tile
            for made in sy.values():
                go(made)

        def sums2():
            for made in sy.values():
                made.wait_recv()
            sums_z[0] = jnp.sum(sums_y[...], axis=0)
            for made in sz.values():
                go(made)

        def sums3():
            for made in sz.values():
                made.wait_recv()
            total = jnp.sum(jnp.sum(sums_z[...], axis=0), keepdims=True)
            factor[...] = jnp.broadcast_to(jnp.sqrt(N / total), factor.shape)

        work = dict(
            own=own, zd=zd, zu=zu, put=put, xfu=xfu, xfd=xfd, xnear=xnear, xlast=xlast, mul=mul,
            s1=s1, s2=s2, s3=s3, s6=s6, rc=rc, rn=rn, re=re, fin=fin,
            sums1=sums1, sums2=sums2, sums3=sums3,
        )
        for name, *args in ORDER[it]:
            with jax.named_scope("_".join([f"i{it}", name, *map(str, args)])):
                work[name](*args)

    for it in range(ITERS):
        iteration(it)
    for made in pending:
        made.wait_send()


def shards(matrix):
    dma = pltpu.SemaphoreType.DMA
    wide = NX * STRIP
    widths = [n * STRIP for _, n in LANES]

    def per_set(*shape):
        return [pltpu.VMEM((ITERS, NZ, *shape, width), F32) for width in widths]

    return pl.pallas_call(
        kernel,
        out_shape=jax.ShapeDtypeStruct((ROWS, STRIP), F32),
        in_specs=[pl.BlockSpec(memory_space=pltpu.VMEM)],
        out_specs=pl.BlockSpec(memory_space=pltpu.VMEM),
        scratch_shapes=[
            pltpu.VMEM((ITERS, NZ, ROWS, STRIP), F32),
            pltpu.VMEM((ITERS, NX, ROWS, STRIP), F32),
            pltpu.VMEM((ROWS, NZ * STRIP), BF),
            pltpu.VMEM((ROWS, NZ * STRIP), BF),
            pltpu.VMEM((ROWS, wide), BF),
            pltpu.VMEM((ROWS, wide), BF),
            pltpu.VMEM((NZ * STRIP, wide), BF),
            pltpu.VMEM((NZ * STRIP, wide), BF),
            *per_set(NC, SROWS),
            *per_set(SROWS),
            *per_set(SROWS),
            *per_set(SROWS),
            *per_set(SROWS),
            *per_set(SROWS),
            *per_set(NC, SROWS),
            pltpu.VMEM((ITERS, NX, ROWS, STRIP), F32),
            pltpu.VMEM((ITERS, 4, HALF, STRIP), F32),
            pltpu.VMEM((ITERS, 2, HALF, STRIP), F32),
            pltpu.VMEM((8, 128), F32),
            pltpu.VMEM((NY * NC, 8, 128), F32),
            pltpu.VMEM((NZ, 8, 128), F32),
            dma((ITERS, NZ, 2)),
            dma((ITERS, NZ, 2)),
            dma((ITERS, 12)),
            dma((ITERS, 12)),
            dma((ITERS, len(GROUPS), len(SETS), 6)),
            dma((ITERS, len(GROUPS), len(SETS), 6)),
            dma((NY * NC + NZ,)),
            dma((NY * NC + NZ,)),
        ],
        compiler_params=pltpu.CompilerParams(
            collective_id=0, has_side_effects=True, vmem_limit_bytes=56 * 1024 * 1024
        ),
    )(matrix)


def solution(mesh):
    grid = Mesh(mesh.devices.reshape(NY, NC, NX, NZ), ("y", "c", "x", "z"))
    spec = P(("y", "c"), ("x", "z"))
    return jax.shard_map(shards, mesh=grid, in_specs=(spec,), out_specs=spec, check_vma=False)
```

```python
import jax
import jax.numpy as jnp
from jax import lax
from jax.experimental import pallas as pl
from jax.experimental.pallas import tpu as pltpu
from jax.sharding import Mesh
from jax.sharding import PartitionSpec as P

N = 4096
ITERS = 2
NY, NC, NX, NZ = 4, 2, 4, 8
ROWS = N // (NY * NC)
STRIP = N // (NX * NZ)
HALF = ROWS // 2
PIECES = 4
PIECE = ROWS // PIECES
SROWS = STRIP // NC
SHALF = SROWS // 2
SQUARTER = SROWS // 4
GROUPS = ((0, 1), (1, 2), (3, 2), (5, 2), (7, 1))
SETS = ((2,), (1, 3), (0,))
LANES = ((0, 1), (1, 2), (3, 1))
BF = jnp.bfloat16
F32 = jnp.float32
THREE_STEPS = 12
ORDER = (
    (
        ("oxu", 2), ("oxd", 1), ("ozu", 2), ("oxd", 3), ("ozu", 1), ("ozd", 0), ("put", 0), ("oxu", 0), ("ozd", 2),
        ("ozu", 0), ("ozd", 1), ("oxu", 1), ("ozu", 3), ("ozd", 3), ("oxd", 2), ("oxu", 3), ("oxd", 0),
        ("mul", 0, 2), ("s1", 0, 2), ("zd", 1, 0, 0), ("zu", 2, 2, 0), ("s2", 0, 2), ("zu", 2, 1, 0),
        ("zd", 1, 2, 0), ("xfu", 0), ("xfd", 3), ("zd", 1, 1, 0), ("zu", 2, 0, 0), ("xfd", 2), ("xfu", 1),
        ("s3", 0, 2), ("zd", 1, 3, 0), ("put", 1), ("zu", 2, 3, 0), ("put", 2), ("mul", 1, 2), ("xnear",),
        ("mul", 1, 1), ("mul", 0, 1), ("zu", 4, 2, 0), ("zd", 3, 0, 0), ("s1", 1, 2), ("s4", 0, 2), ("s1", 1, 1),
        ("s1", 0, 1), ("zd", 3, 2, 0), ("zu", 4, 1, 0), ("xlast",), ("mul", 1, 0), ("mul", 0, 0), ("sums1",),
        ("zu", 4, 0, 0), ("zd", 3, 1, 0), ("s1", 1, 0), ("s2", 1, 2), ("s1", 0, 0), ("zd", 3, 3, 0),
        ("zu", 4, 3, 0), ("put", 4), ("put", 3), ("mul", 2), ("s2", 1, 1), ("s2", 0, 1), ("zu", 6, 2, 0),
        ("zd", 5, 0, 0), ("s1", 2, 0), ("sums2",), ("s2", 1, 0), ("s1", 2, 1), ("s1", 2, 2), ("s3", 1, 2),
        ("zd", 5, 2, 0), ("zu", 6, 1, 0), ("s2", 0, 0), ("zu", 6, 0, 0), ("s3", 1, 1), ("zd", 5, 1, 0),
        ("s3", 0, 1), ("s2", 2, 0), ("s3", 1, 0), ("zd", 5, 3, 0), ("put", 5), ("zu", 6, 3, 0), ("put", 6),
        ("mul", 3), ("s2", 2, 1), ("s2", 2, 2), ("s4", 1, 2), ("s3", 0, 0), ("s1", 3, 0), ("s4", 1, 1),
        ("s1", 3, 1), ("s1", 3, 2), ("s4", 0, 1), ("s3", 2, 0), ("sums3",), ("s4", 1, 0), ("put", 7), ("mul", 4),
        ("s3", 2, 1), ("s3", 2, 2), ("s4", 0, 0), ("s2", 3, 0), ("s1", 4, 0), ("s1", 4, 1), ("s1", 4, 2),
        ("s2", 3, 1), ("s6", 0), ("s4", 2, 0), ("s6", 1), ("s4", 2, 1), ("s2", 3, 2), ("s6", 2, 0), ("s3", 3, 0),
        ("s4", 2, 2), ("s2", 4, 0), ("s6", 2, 1), ("s2", 4, 1), ("s2", 4, 2), ("s6", 2, 2), ("s3", 3, 1),
        ("s3", 3, 2), ("s4", 3, 0), ("s3", 4, 0), ("s6", 3, 0), ("s6", 4, 0), ("rc", 0), ("s3", 4, 2), ("s3", 4, 1),
        ("rc", 1), ("s4", 3, 1), ("s4", 3, 2), ("s6", 3, 1), ("s6", 4, 1), ("rn", 1), ("rn", 0), ("s6", 3, 2),
        ("s6", 4, 2), ("re", 0), ("re", 1), ("fin", 0), ("fin", 1),
    ),
    (
        ("oxd", 2), ("ozu", 2), ("oxu", 2), ("oxu", 0), ("ozu", 0), ("oxd", 0), ("ozd", 2), ("ozd", 0), ("ozd", 1),
        ("oxd", 3), ("oxu", 1), ("ozd", 3), ("ozu", 1), ("oxd", 1), ("put", 0), ("mul", 0, 2), ("oxu", 3),
        ("ozu", 3), ("s1", 0, 2), ("zd", 1, 2, 0), ("zu", 2, 2, 0), ("xfd", 2), ("zd", 1, 0, 0), ("zu", 2, 0, 0),
        ("xfu", 0), ("s2", 0, 2), ("zd", 1, 1, 0), ("zu", 2, 1, 0), ("xfd", 3), ("xfu", 1), ("zd", 1, 3, 0),
        ("put", 1), ("zu", 2, 3, 0), ("put", 2), ("mul", 1, 2), ("xnear",), ("mul", 0, 1), ("s3", 0, 2),
        ("mul", 1, 1), ("zd", 3, 2, 0), ("zu", 4, 2, 0), ("s1", 1, 2), ("s1", 0, 1), ("zd", 3, 0, 0),
        ("zu", 4, 0, 0), ("s1", 1, 1), ("xlast",), ("mul", 0, 0), ("mul", 1, 0), ("s4", 0, 2), ("zu", 4, 1, 0),
        ("zd", 3, 1, 0), ("s1", 0, 0), ("s2", 1, 2), ("s1", 1, 0), ("s2", 0, 1), ("zu", 4, 3, 0), ("put", 4),
        ("zd", 3, 3, 0), ("put", 3), ("mul", 2), ("s2", 1, 1), ("zu", 6, 2, 0), ("zd", 5, 2, 0), ("s2", 0, 0),
        ("s1", 2, 0), ("s1", 2, 1), ("s1", 2, 2), ("s3", 1, 2), ("zu", 6, 0, 0), ("s2", 1, 0), ("zd", 5, 0, 0),
        ("s3", 0, 1), ("zu", 6, 1, 0), ("s3", 1, 1), ("zd", 5, 1, 0), ("s3", 0, 0), ("s2", 2, 0), ("zd", 5, 3, 0),
        ("put", 5), ("zu", 6, 3, 0), ("put", 6), ("mul", 3), ("s2", 2, 1), ("s2", 2, 2), ("s4", 1, 2), ("s3", 1, 0),
        ("s4", 0, 1), ("s1", 3, 0), ("s1", 3, 1), ("s4", 1, 1), ("s1", 3, 2), ("s4", 0, 0), ("s3", 2, 0),
        ("put", 7), ("mul", 4), ("s3", 2, 1), ("s6", 0), ("s3", 2, 2), ("s4", 1, 0), ("s2", 3, 0), ("s1", 4, 0),
        ("s1", 4, 1), ("s1", 4, 2), ("s2", 3, 1), ("s2", 3, 2), ("s6", 1), ("s4", 2, 0), ("s4", 2, 1), ("s4", 2, 2),
        ("s3", 3, 0), ("s2", 4, 0), ("s6", 2, 0), ("s6", 2, 2), ("s2", 4, 1), ("s6", 2, 1), ("s3", 3, 1),
        ("s2", 4, 2), ("s3", 3, 2), ("s4", 3, 0), ("s3", 4, 0), ("s6", 3, 0), ("s6", 4, 0), ("rc", 0), ("rc", 1),
        ("s3", 4, 1), ("s4", 3, 1), ("s3", 4, 2), ("s4", 3, 2), ("s6", 3, 1), ("s6", 4, 1), ("rn", 0), ("rn", 1),
        ("s6", 3, 2), ("s6", 4, 2), ("re", 0), ("re", 1), ("fin", 0), ("fin", 1),
    ),
)


def split(value):
    high = value.astype(BF)
    return high, (value - high.astype(F32)).astype(BF)


def three(dim, a, b):
    a = jnp.concatenate([a[0], a[1], a[0]], axis=dim)
    b = jnp.concatenate([b[0], b[0], b[1]], axis=0)
    return lax.dot_general(a, b, (((dim,), (0,)), ((), ())), preferred_element_type=F32)


def lanes_of(s):
    first, n = LANES[s]
    return slice(first * STRIP, (first + n) * STRIP)


def kernel(m_ref, o_ref, block, panel, block_hi, block_lo, panel_hi, panel_lo, square_hi, square_lo, *refs):
    ns = len(SETS)
    part, from_core, mine, first_in, ours, second_in, square = (refs[k * ns : (k + 1) * ns] for k in range(7))
    (
        cube, x_chain, x_ended, factor, sums_y, sums_z, out,
        z_send, z_recv, x_send, x_recv, r_send, r_recv, g_send, g_recv, s_send, s_recv, local_sem,
    ) = refs[7 * ns :]
    y, c, x, z = (lax.axis_index(name) for name in ("y", "c", "x", "z"))

    def turn(name, here, by, size):
        return {name: lax.rem(here + by, size)}

    up_z, down_z = turn("z", z, 1, NZ), turn("z", z, NZ - 1, NZ)
    up_x, down_x = turn("x", x, 1, NX), turn("x", x, NX - 1, NX)
    odd = lax.rem(y, 2)
    y_near, y_far = turn("y", y, NY + 1 - 2 * odd, NY), turn("y", y, NY - 1 + 2 * odd, NY)
    other_core = {"c": 1 - c}
    z_peers = [turn("z", z, d, NZ) for d in range(1, NZ)]
    y_peers = [{"y": lax.rem(y + d, NY), "c": lax.rem(c + e, NC)} for d in range(NY) for e in range(NC)][1:]

    barrier = pltpu.get_barrier_semaphore()
    peers = [up_x, down_x, *z_peers, *y_peers]
    for peer in peers:
        pl.semaphore_signal(barrier, inc=1, device_id=peer, device_id_type=pl.DeviceIdType.MESH)
    fetch = pltpu.make_async_copy(m_ref, block.at[0, 0], local_sem.at[0])
    fetch.start()
    fetch.wait()
    pl.semaphore_wait(barrier, len(peers))

    def copy(src, dst, send, recv, peer):
        return pltpu.make_async_remote_copy(
            src_ref=src, dst_ref=dst, send_sem=send, recv_sem=recv,
            device_id=peer, device_id_type=pl.DeviceIdType.MESH,
        )

    def go(made):
        made.start()

    def all_sent(ref, sem):
        copy(ref, ref, sem, local_sem.at[5], up_x).wait_send()

    low, high = pl.ds(0, SHALF), pl.ds(SHALF, SHALF)
    gray, top = lax.rem(lax.div(y + 1, 2), 2), lax.div(y, 2)

    def sub(half, which):
        return pl.ds(pl.multiple_of(half * SHALF + which * SQUARTER, SQUARTER), SQUARTER)

    stored = []

    def iteration(it):
        block_i, panel_i, cube_i = block.at[it], panel.at[it], cube.at[it]

        def piece_of(q):
            return pl.ds(q * PIECE, PIECE)

        def z_copy(src, dst, q, peer):
            return copy(
                block_i.at[src, piece_of(q)], block_i.at[dst, piece_of(q)],
                z_send.at[it], z_recv.at[it, dst, q], peer,
            )

        every_piece, upper_pieces, lower_pieces = range(PIECES), (0, 1), (2, 3)
        ups = {(p, q): z_copy(max(p - 2, 0), p, q, up_z) for p in (2, 4, 6) for q in every_piece}
        downs = {(p, q): z_copy(max(p - 2, 0), p, q, down_z) for p in (1, 3, 5) for q in every_piece}
        ups.update({(8, q): z_copy(6, 7, q, up_z) for q in upper_pieces})
        downs.update({(7, q): z_copy(5, 7, q, down_z) for q in lower_pieces})

        def x_copy(src, dst, q, peer):
            return copy(
                src.at[piece_of(q)], panel_i.at[dst, piece_of(q)], x_send.at[it], x_recv.at[it, dst, q], peer
            )

        x_up = [x_copy(block_i.at[0], 3, q, up_x) for q in every_piece]
        x_down = [x_copy(block_i.at[0], 1, q, down_x) for q in every_piece]
        x_far = [x_copy(panel_i.at[3], 2, q, up_x) for q in upper_pieces]
        x_far += [x_copy(panel_i.at[1], 2, q, down_x) for q in lower_pieces]

        def put_panel(slot, value):
            at = {2: 0, 1: 1, 3: 2, 0: 3}[slot]
            columns = slice(at * STRIP, (at + 1) * STRIP)
            panel_hi[:, columns], panel_lo[:, columns] = split(value)

        def ozu(q):
            go(ups[2, q])

        def ozd(q):
            go(downs[1, q])

        def oxu(q):
            go(x_up[q])

        def oxd(q):
            go(x_down[q])

        def zd(pos, piece, _):
            downs[pos, piece].wait_recv()
            if (pos + 2, piece) in downs:
                go(downs[pos + 2, piece])

        def zu(pos, piece, _):
            ups[pos, piece].wait_recv()
            if (pos + 2, piece) in ups:
                go(ups[pos + 2, piece])

        def put(pos):
            if pos == 7:
                for q in upper_pieces:
                    ups[8, q].wait_recv()
                for q in lower_pieces:
                    downs[7, q].wait_recv()
            columns = slice(pos * STRIP, (pos + 1) * STRIP)
            value = block[it, pos]
            block_hi[:, columns], block_lo[:, columns] = split(value)
            if pos == 0:
                put_panel(0, value)

        def xfu(q):
            x_up[q].wait_recv()
            go(x_far[q])

        def xfd(q):
            x_down[q].wait_recv()
            go(x_far[q])

        def xnear():
            for q in lower_pieces:
                x_up[q].wait_recv()
            for q in upper_pieces:
                x_down[q].wait_recv()
            put_panel(3, panel[it, 3])
            put_panel(1, panel[it, 1])

        def xlast():
            for q in every_piece:
                x_far[q].wait_recv()
            put_panel(2, panel[it, 2])

        def unit(g, s):
            run = pl.ds(*GROUPS[g])
            every = slice(None)

            three_steps = g * ns + s < THREE_STEPS

            def made(k, src, dst, peer):
                to = 0 if k in (0, 5) else 1 if not three_steps else 2 + {1: 0, 2: 0, 3: 1, 4: 1, 6: 2, 7: 2}[k]
                return copy(src, dst, g_send.at[it, s, to], g_recv.at[it, g, s, k], peer)

            def rows(ref, which):
                return ref[s].at[it, run, which]

            sums = square[s].at[it, run, c]
            cs = dict(
                core=made(0, part[s].at[it, run, 1 - c], from_core[s].at[it, run], other_core),
                join=made(5, sums, sums, other_core),
            )
            if three_steps:
                one, two = (sub(0, 1 - gray), sub(1, 1 - top)), (sub(0, gray), sub(1, top))
                low_sums, high_sums = square[s].at[it, run, c, two[0]], square[s].at[it, run, c, two[1]]
                cs["low_three"] = made(6, low_sums, low_sums, y_near)
                cs["high_three"] = made(7, high_sums, high_sums, y_far)
            else:
                one = two = (low, high)
            cs["low_one"] = made(1, rows(mine, one[0]), rows(first_in, one[0]), y_near)
            cs["high_one"] = made(2, rows(mine, one[1]), rows(first_in, one[1]), y_far)
            cs["low_two"] = made(3, rows(ours, two[0]), rows(second_in, two[0]), y_far)
            cs["high_two"] = made(4, rows(ours, two[1]), rows(second_in, two[1]), y_near)
            cs["kept"] = two
            return cs

        units = {(g, s): unit(g, s) for g in range(len(GROUPS)) for s in range(ns)}

        def strips(g):
            first, n = GROUPS[g]
            return range(first, first + n)

        def factors(g):
            first, n = GROUPS[g]
            columns = slice(first * STRIP, (first + n) * STRIP)
            return block_hi[:, columns], block_lo[:, columns]

        def mul(g, *which):
            first, n = GROUPS[g]
            columns = lanes_of(which[0]) if which else slice(0, NX * STRIP)
            got = three(0, factors(g), (panel_hi[:, columns], panel_lo[:, columns]))
            for s in which or range(ns):
                piece = got if which else got[:, lanes_of(s)]
                part[s][it, first : first + n] = piece.reshape(n, NC, SROWS, piece.shape[1])
                go(units[g, s]["core"])

        def s1(g, s):
            cs = units[g, s]
            cs["core"].wait_recv()
            for p in strips(g):
                mine[s][it, p] = part[s][it, p, c] + from_core[s][it, p]
            go(cs["low_one"])
            go(cs["high_one"])

        def s2(g, s):
            cs = units[g, s]
            for half, kept in zip(("low", "high"), cs["kept"]):
                cs[half + "_one"].wait_recv()
                for p in strips(g):
                    ours[s][it, p, kept] = mine[s][it, p, kept] + first_in[s][it, p, kept]
                go(cs[half + "_two"])

        def s3(g, s):
            cs = units[g, s]
            for half, kept in zip(("low", "high"), cs["kept"]):
                cs[half + "_two"].wait_recv()
                for p in strips(g):
                    square[s][it, p, c, kept] = ours[s][it, p, kept] + second_in[s][it, p, kept]
                if half + "_three" in cs:
                    go(cs[half + "_three"])
            if "low_three" not in cs:
                go(cs["join"])

        def s4(g, s):
            cs = units[g, s]
            cs["low_three"].wait_recv()
            cs["high_three"].wait_recv()
            go(cs["join"])

        def s6(g, *which):
            first, n = GROUPS[g]
            rows = slice(first * STRIP, (first + n) * STRIP)
            todo = which or range(ns)
            for s in todo:
                units[g, s]["join"].wait_recv()
                value = square[s][it, first : first + n]
                value = value.reshape(n * STRIP, value.shape[-1])
                if it == 0:
                    f = factor[0:1, 0:1]
                    value = value * (f * f)
                square_hi[rows, lanes_of(s)], square_lo[rows, lanes_of(s)] = split(value)
            columns = lanes_of(which[0]) if which else slice(0, NX * STRIP)
            got = three(1, factors(g), (square_hi[rows, columns], square_lo[rows, columns]))
            for k, slot in enumerate([slot for s in todo for slot in SETS[s]]):
                piece = got[:, k * STRIP : (k + 1) * STRIP]
                if first == 0:
                    cube[it, slot] = piece
                else:
                    cube[it, slot] += piece

        def reduce_copies(r):
            upper, lower = pl.ds(r * PIECE, PIECE), pl.ds(HALF + r * PIECE, PIECE)

            def made(k, slot, rows, dst, peer):
                return copy(cube_i.at[slot, rows], dst, r_send.at[it], r_recv.at[it, r, k], peer)

            return dict(
                chain_up=made(0, 2, upper, x_chain.at[it, r, 0], up_x),
                chain_down=made(1, 2, lower, x_chain.at[it, r, 1], down_x),
                near_down=made(2, 3, upper, x_chain.at[it, r, 2], down_x),
                near_up=made(3, 1, lower, x_chain.at[it, r, 3], up_x),
                end_up=made(4, 1, upper, x_ended.at[it, r, 0], up_x),
                end_down=made(5, 3, lower, x_ended.at[it, r, 1], down_x),
                rows=(upper, lower),
            )

        reduces = [reduce_copies(r) for r in range(2)]

        def rc(r):
            go(reduces[r]["chain_up"])
            go(reduces[r]["chain_down"])

        def rn(r):
            go(reduces[r]["near_up"])
            go(reduces[r]["near_down"])

        def re(r):
            cs = reduces[r]
            for k, (slot, way) in enumerate(((1, "up"), (3, "down"))):
                cs["chain_" + way].wait_recv()
                cube[it, slot, cs["rows"][k]] += x_chain[it, r, k]
                go(cs["end_" + way])

        def fin(r):
            cs = reduces[r]
            cs["near_down"].wait_recv()
            cs["near_up"].wait_recv()
            for k, way in enumerate(("up", "down")):
                cs["end_" + way].wait_recv()
                rows = cs["rows"][k]
                product = cube[it, 0, rows] + (x_ended[it, r, k] + x_chain[it, r, 2 + k])
                value = block[it, 0, rows]
                if it == 0:
                    f = factor[0:1, 0:1]
                    new = (1.5 * f) * value - (0.5 * f) * product
                else:
                    new = 1.5 * value - 0.5 * product
                if it == ITERS - 1:
                    out[rows] = new
                    store = pltpu.make_async_copy(out.at[rows], o_ref.at[rows], local_sem.at[1 + 2 * r + k])
                    store.start()
                    stored.append(store)
                else:
                    block[it + 1, 0, rows] = new

        sy, sz = {}, {}
        if it == 0:
            for k, peer in enumerate(y_peers, 1):
                sy[k] = copy(sums_y.at[0], sums_y.at[k], s_send.at[0], s_recv.at[k], peer)
            for k, peer in enumerate(z_peers, 1):
                sz[k] = copy(sums_z.at[0], sums_z.at[k], s_send.at[1], s_recv.at[8 + k], peer)

        def sums1():
            tile = jnp.zeros((8, 128), F32)
            for v in (block[it, 0], panel[it, 1], panel[it, 2], panel[it, 3]):
                v = v.reshape(ROWS // 8, 8, STRIP)
                tile = tile + jnp.sum(v * v, axis=0)
            sums_y[0] = tile
            for made in sy.values():
                go(made)

        def sums2():
            for made in sy.values():
                made.wait_recv()
            sums_z[0] = jnp.sum(sums_y[...], axis=0)
            for made in sz.values():
                go(made)

        def sums3():
            for made in sz.values():
                made.wait_recv()
            total = jnp.sum(jnp.sum(sums_z[...], axis=0), keepdims=True)
            factor[...] = jnp.broadcast_to(jnp.sqrt(N / total), factor.shape)

        work = dict(
            ozu=ozu, ozd=ozd, oxu=oxu, oxd=oxd, zd=zd, zu=zu, put=put, xfu=xfu, xfd=xfd, xnear=xnear, xlast=xlast, mul=mul,
            s1=s1, s2=s2, s3=s3, s4=s4, s6=s6, rc=rc, rn=rn, re=re, fin=fin,
            sums1=sums1, sums2=sums2, sums3=sums3,
        )
        for name, *args in ORDER[it]:
            with jax.named_scope("_".join([f"i{it}", name, *map(str, args)])):
                work[name](*args)

    for it in range(ITERS):
        iteration(it)
    for it in range(ITERS):
        all_sent(block.at[it, pl.ds(0, NZ - 1)], z_send.at[it])
        all_sent(panel.at[it, pl.ds(0, NX - 1)], x_send.at[it])
        all_sent(cube.at[it, pl.ds(0, NX - 1)], r_send.at[it])
        for s in range(ns):
            slow = sum(n for g, (_, n) in enumerate(GROUPS) if g * ns + s < THREE_STEPS)
            all_sent(square[s].at[it], g_send.at[it, s, 0])
            if slow < NZ:
                all_sent(square[s].at[it, pl.ds(0, NZ - slow)], g_send.at[it, s, 1])
            for k in range(3 if slow else 0):
                all_sent(mine[s].at[it, pl.ds(0, slow), low], g_send.at[it, s, 2 + k])
    all_sent(sums_y.at[pl.ds(1, NY * NC - 1)], s_send.at[0])
    all_sent(sums_z.at[pl.ds(1, NZ - 1)], s_send.at[1])
    for store in stored:
        store.wait()


def shards(matrix):
    dma = pltpu.SemaphoreType.DMA
    wide = NX * STRIP
    widths = [n * STRIP for _, n in LANES]

    def per_set(*shape):
        return [pltpu.VMEM((ITERS, NZ, *shape, width), F32) for width in widths]

    return pl.pallas_call(
        kernel,
        out_shape=jax.ShapeDtypeStruct((ROWS, STRIP), F32),
        in_specs=[pl.BlockSpec(memory_space=pltpu.HBM)],
        out_specs=pl.BlockSpec(memory_space=pltpu.HBM),
        scratch_shapes=[
            pltpu.VMEM((ITERS, NZ, ROWS, STRIP), F32),
            pltpu.VMEM((ITERS, NX, ROWS, STRIP), F32),
            pltpu.VMEM((ROWS, NZ * STRIP), BF),
            pltpu.VMEM((ROWS, NZ * STRIP), BF),
            pltpu.VMEM((ROWS, wide), BF),
            pltpu.VMEM((ROWS, wide), BF),
            pltpu.VMEM((NZ * STRIP, wide), BF),
            pltpu.VMEM((NZ * STRIP, wide), BF),
            *per_set(NC, SROWS),
            *per_set(SROWS),
            *per_set(SROWS),
            *per_set(SROWS),
            *per_set(SROWS),
            *per_set(SROWS),
            *per_set(NC, SROWS),
            pltpu.VMEM((ITERS, NX, ROWS, STRIP), F32),
            pltpu.VMEM((ITERS, 2, 4, PIECE, STRIP), F32),
            pltpu.VMEM((ITERS, 2, 2, PIECE, STRIP), F32),
            pltpu.VMEM((8, 128), F32),
            pltpu.VMEM((NY * NC, 8, 128), F32),
            pltpu.VMEM((NZ, 8, 128), F32),
            pltpu.VMEM((ROWS, STRIP), F32),
            dma((ITERS,)),
            dma((ITERS, NZ, PIECES)),
            dma((ITERS,)),
            dma((ITERS, NX, PIECES)),
            dma((ITERS,)),
            dma((ITERS, 2, 6)),
            dma((ITERS, len(SETS), 5)),
            dma((ITERS, len(GROUPS), len(SETS), 8)),
            dma((2,)),
            dma((NY * NC + NZ,)),
            dma((6,)),
        ],
        compiler_params=pltpu.CompilerParams(
            collective_id=0, has_side_effects=True, vmem_limit_bytes=56 * 1024 * 1024
        ),
    )(matrix)


def solution(mesh):
    grid = Mesh(mesh.devices.reshape(NY, NC, NX, NZ), ("y", "c", "x", "z"))
    spec = P(("y", "c"), ("x", "z"))
    return jax.shard_map(shards, mesh=grid, in_specs=(spec,), out_specs=spec, check_vma=False)
```

```python
import jax
import jax.numpy as jnp
from jax import lax
from jax.experimental import pallas as pl
from jax.experimental.pallas import tpu as pltpu
from jax.sharding import Mesh
from jax.sharding import PartitionSpec as P

N = 4096
ITERS = 2
NY, NC, NX, NZ = 4, 2, 4, 8
ROWS = N // (NY * NC)
STRIP = N // (NX * NZ)
HALF = ROWS // 2
PIECES = 4
PIECE = ROWS // PIECES
SROWS = STRIP // NC
SHALF = SROWS // 2
SQUARTER = SROWS // 4
GROUPS = ((0, 1), (1, 2), (3, 2), (5, 2), (7, 1))
SETS = ((2,), (1, 3), (0,))
LANES = ((0, 1), (1, 2), (3, 1))
BF = jnp.bfloat16
F32 = jnp.float32
MERGED = (0,)
THREE_STEPS = 12
ORDER = (
    (
        ("own", 0), ("put", 0), ("mul", 0, 2), ("own", 1), ("s1", 0, 2), ("zz", 0, 0), ("xf", 0), ("s2", 0, 2),
        ("zz", 0, 1), ("zz", 0, 2), ("xf", 1), ("s3", 0, 2), ("zz", 0, 3), ("put", 1), ("put", 2), ("mul", 1, 2),
        ("xnear",), ("mul", 1, 1), ("mul", 0, 1), ("zz", 1, 0), ("s1", 1, 2), ("s4", 0, 2), ("s1", 1, 1),
        ("zz", 1, 1), ("s1", 0, 1), ("xlast",), ("sums1",), ("mul", 0, 0), ("mul", 1, 0), ("zz", 1, 2),
        ("s1", 0, 0), ("s2", 1, 2), ("s1", 1, 0), ("zz", 1, 3), ("put", 3), ("put", 4), ("mul", 2), ("s2", 1, 1),
        ("s2", 0, 1), ("zz", 2, 0), ("sums2",), ("s2", 0, 0), ("s1", 2, 0), ("s1", 2, 1), ("s1", 2, 2),
        ("s3", 1, 2), ("zz", 2, 1), ("s2", 1, 0), ("zz", 2, 2), ("s3", 1, 1), ("s3", 0, 1), ("s3", 0, 0),
        ("s2", 2, 0), ("zz", 2, 3), ("put", 6), ("put", 5), ("mul", 3), ("s2", 2, 1), ("s2", 2, 2), ("s4", 1, 2),
        ("s3", 1, 0), ("s1", 3, 0), ("s4", 1, 1), ("sums3",), ("s4", 0, 1), ("s1", 3, 1), ("s1", 3, 2),
        ("s4", 0, 0), ("put", 7), ("mul", 4), ("s3", 2, 0), ("s6", 0), ("s3", 2, 1), ("s6", 1, 1), ("s6", 1, 2),
        ("s2", 3, 0), ("s4", 1, 0), ("s1", 4, 0), ("s1", 4, 2), ("s3", 2, 2), ("s1", 4, 1), ("s2", 3, 1),
        ("s2", 3, 2), ("s6", 1, 0), ("s4", 2, 0), ("s4", 2, 1), ("s3", 3, 0), ("s6", 2, 0), ("s2", 4, 0),
        ("s2", 4, 2), ("s6", 2, 1), ("s4", 2, 2), ("s2", 4, 1), ("s3", 3, 1), ("s6", 2, 2), ("s3", 3, 2),
        ("s4", 3, 0), ("s3", 4, 0), ("s3", 4, 2), ("s6", 3, 0), ("s6", 4, 0), ("rc", 1), ("rc", 0), ("s3", 4, 1),
        ("s4", 3, 1), ("s4", 3, 2), ("s6", 3, 1), ("s6", 4, 1), ("rn", 1), ("rn", 0), ("s6", 3, 2), ("s6", 4, 2),
        ("re", 1), ("re", 0), ("fin", 1), ("fin", 0),
    ),
    (
        ("own", 1), ("put", 0), ("own", 0), ("mul", 0, 2), ("s1", 0, 2), ("zz", 0, 2), ("xf", 1), ("zz", 0, 3),
        ("s2", 0, 2), ("zz", 0, 0), ("xf", 0), ("zz", 0, 1), ("put", 1), ("put", 2), ("mul", 1, 2), ("xnear",),
        ("mul", 0, 1), ("s3", 0, 2), ("mul", 1, 1), ("zz", 1, 2), ("s1", 1, 2), ("s1", 0, 1), ("zz", 1, 3),
        ("s1", 1, 1), ("xlast",), ("mul", 0, 0), ("mul", 1, 0), ("s4", 0, 2), ("zz", 1, 0), ("s1", 0, 0),
        ("s2", 1, 2), ("s1", 1, 0), ("s2", 0, 1), ("zz", 1, 1), ("put", 4), ("put", 3), ("mul", 2), ("s2", 1, 1),
        ("zz", 2, 2), ("s2", 0, 0), ("s1", 2, 0), ("s1", 2, 1), ("s1", 2, 2), ("s3", 1, 2), ("zz", 2, 3),
        ("s2", 1, 0), ("s3", 0, 1), ("zz", 2, 0), ("s3", 1, 1), ("s3", 0, 0), ("s2", 2, 0), ("zz", 2, 1),
        ("put", 5), ("put", 6), ("mul", 3), ("s2", 2, 2), ("s2", 2, 1), ("s4", 1, 2), ("s3", 1, 0), ("s4", 0, 1),
        ("s1", 3, 0), ("s1", 3, 1), ("s1", 3, 2), ("s4", 1, 1), ("s4", 0, 0), ("put", 7), ("mul", 4), ("s3", 2, 0),
        ("s3", 2, 2), ("s6", 0), ("s6", 1, 2), ("s1", 4, 2), ("s1", 4, 0), ("s6", 1, 1), ("s4", 1, 0), ("s2", 3, 0),
        ("s1", 4, 1), ("s3", 2, 1), ("s2", 3, 1), ("s2", 3, 2), ("s6", 1, 0), ("s4", 2, 0), ("s4", 2, 2),
        ("s2", 4, 2), ("s2", 4, 0), ("s6", 2, 0), ("s3", 3, 0), ("s6", 2, 2), ("s2", 4, 1), ("s4", 2, 1),
        ("s3", 3, 1), ("s3", 3, 2), ("s3", 4, 2), ("s6", 2, 1), ("s3", 4, 0), ("s4", 3, 0), ("s3", 4, 1),
        ("s6", 3, 0), ("s6", 4, 0), ("rc", 0), ("rc", 1), ("s4", 3, 1), ("s4", 3, 2), ("s6", 3, 1), ("s6", 4, 1),
        ("rn", 0), ("rn", 1), ("s6", 3, 2), ("s6", 4, 2), ("re", 0), ("re", 1), ("fin", 0), ("fin", 1),
    ),
)


def split(value):
    high = value.astype(BF)
    return high, (value - high.astype(F32)).astype(BF)


def three(dim, a, b):
    a = jnp.concatenate([a[0], a[1], a[0]], axis=dim)
    b = jnp.concatenate([b[0], b[0], b[1]], axis=0)
    return lax.dot_general(a, b, (((dim,), (0,)), ((), ())), preferred_element_type=F32)


def lanes_of(s):
    first, n = LANES[s]
    return slice(first * STRIP, (first + n) * STRIP)


def kernel(m_ref, o_ref, block, panel, block_hi, block_lo, panel_hi, panel_lo, square_hi, square_lo, *refs):
    ns = len(SETS)
    part, from_core, mine, first_in, ours, second_in, square = (refs[k * ns : (k + 1) * ns] for k in range(7))
    (
        cube, x_chain, x_ended, factor, sums_y, sums_z,
        z_send, z_recv, x_send, x_recv, r_send, r_recv, g_send, g_recv, s_send, s_recv, local_sem,
    ) = refs[7 * ns :]
    y, c, x, z = (lax.axis_index(name) for name in ("y", "c", "x", "z"))

    def turn(name, here, by, size):
        return {name: lax.rem(here + by, size)}

    up_z, down_z = turn("z", z, 1, NZ), turn("z", z, NZ - 1, NZ)
    up_x, down_x = turn("x", x, 1, NX), turn("x", x, NX - 1, NX)
    odd = lax.rem(y, 2)
    y_near, y_far = turn("y", y, NY + 1 - 2 * odd, NY), turn("y", y, NY - 1 + 2 * odd, NY)
    other_core = {"c": 1 - c}
    z_peers = [turn("z", z, d, NZ) for d in range(1, NZ)]
    y_peers = [{"y": lax.rem(y + d, NY), "c": lax.rem(c + e, NC)} for d in range(NY) for e in range(NC)][1:]

    barrier = pltpu.get_barrier_semaphore()
    peers = [up_x, down_x, up_z, down_z, y_near, y_far, other_core]
    for peer in peers:
        pl.semaphore_signal(barrier, inc=1, device_id=peer, device_id_type=pl.DeviceIdType.MESH)
    fetch = pltpu.make_async_copy(m_ref, block.at[0, 0], local_sem.at[0])
    fetch.start()
    with jax.named_scope("fetch"):
        fetch.wait()
    with jax.named_scope("barrier"):
        pl.semaphore_wait(barrier, len(peers))

    def copy(src, dst, send, recv, peer):
        return pltpu.make_async_remote_copy(
            src_ref=src, dst_ref=dst, send_sem=send, recv_sem=recv,
            device_id=peer, device_id_type=pl.DeviceIdType.MESH,
        )

    def go(made):
        made.start()

    def all_sent(ref, sem):
        copy(ref, ref, sem, local_sem.at[2], up_x).wait_send()

    def all_here(ref, sem):
        copy(ref, ref, local_sem.at[2], sem, up_x).wait_recv()

    low, high = pl.ds(0, SHALF), pl.ds(SHALF, SHALF)
    gray, top = lax.rem(lax.div(y + 1, 2), 2), lax.div(y, 2)

    def sub(half, which):
        return pl.ds(pl.multiple_of(half * SHALF + which * SQUARTER, SQUARTER), SQUARTER)


    def iteration(it):
        block_i, panel_i, cube_i = block.at[it], panel.at[it], cube.at[it]

        def piece_of(q):
            return pl.ds(q * PIECE, PIECE)

        def z_copy(src, dst, q, pair, i, peer):
            return copy(
                block_i.at[src, piece_of(q)], block_i.at[dst, piece_of(q)], z_send.at[it], z_recv.at[it, pair, i], peer
            )

        up_order, down_order = (0, 2, 1, 3), (2, 0, 3, 1)
        ups, downs = {}, {}
        for pair in range(3):
            for i in range(PIECES):
                q, d = up_order[i], down_order[i]
                ups[pair, i] = z_copy(max(2 * pair, 0), 2 * pair + 2, q, pair, i, up_z)
                downs[pair, i] = z_copy(max(2 * pair - 1, 0), 2 * pair + 1, d, pair, i, down_z)
        for i in (0, 2):
            ups[3, i] = z_copy(6, 7, up_order[i], 3, 0, up_z)
            downs[3, i] = z_copy(5, 7, down_order[i], 3, 0, down_z)

        def x_copy(src, dst, q, k, peer):
            return copy(src.at[piece_of(q)], panel_i.at[dst, piece_of(q)], x_send.at[it], x_recv.at[it, k], peer)

        x_up = [x_copy(block_i.at[0], 3, q, (0, 1, 2, 2)[q], up_x) for q in range(PIECES)]
        x_down = [x_copy(block_i.at[0], 1, q, (2, 2, 0, 1)[q], down_x) for q in range(PIECES)]
        x_far = [x_copy(panel_i.at[3 - 2 * (q // 2)], 2, q, 3, (up_x, down_x)[q // 2]) for q in range(PIECES)]
        pair_rows = pl.ds(0, 2 * PIECE)

        def put_panel(slot, value):
            at = {2: 0, 1: 1, 3: 2, 0: 3}[slot]
            columns = slice(at * STRIP, (at + 1) * STRIP)
            panel_hi[:, columns], panel_lo[:, columns] = split(value)

        def own(h):
            for q, d in ((h, 2 + h), (2 + h, h)):
                go(x_up[q])
                go(x_down[d])
                i = up_order.index(q)
                go(ups[0, i])
                go(downs[0, i])

        def zz(pair, i):
            all_here(block_i.at[0, pair_rows], z_recv.at[it, pair, i])
            if (pair + 1, i) in ups:
                go(ups[pair + 1, i])
                go(downs[pair + 1, i])

        def put(pos):
            if pos == 7:
                all_here(block_i.at[0], z_recv.at[it, 3, 0])
            columns = slice(pos * STRIP, (pos + 1) * STRIP)
            value = block[it, pos]
            block_hi[:, columns], block_lo[:, columns] = split(value)
            if pos == 0:
                put_panel(0, value)

        def xf(i):
            all_here(block_i.at[0, pair_rows], x_recv.at[it, i])
            go(x_far[i])
            go(x_far[2 + i])

        def xnear():
            all_here(block_i.at[0], x_recv.at[it, 2])
            put_panel(3, panel[it, 3])
            put_panel(1, panel[it, 1])

        def xlast():
            all_here(block_i.at[0], x_recv.at[it, 3])
            put_panel(2, panel[it, 2])

        unit_sems = {(g, s): 5 * (g * ns + s) for g in range(len(GROUPS)) for s in range(ns)}

        def unit(g, s):
            run = pl.ds(*GROUPS[g])
            every = slice(None)

            three_steps = g * ns + s < THREE_STEPS

            def made(k, src, dst, peer):
                kind = (0, 1, 1, 2, 2, 4, 3, 3)[k]
                to = 0 if kind in (0, 4) else 3 if not three_steps else 2 if kind == 2 else 1
                wide = 0 if kind == 4 and g in MERGED else s
                return copy(src, dst, g_send.at[it, to], g_recv.at[it, unit_sems[g, wide] + kind], peer)

            def rows(ref, which):
                return ref[s].at[it, run, which]

            sums = square[s].at[it, run, c]
            cs = dict(
                core=made(0, part[s].at[it, run, 1 - c], from_core[s].at[it, run], other_core),
                join=made(5, sums, sums, other_core),
            )
            if three_steps:
                one, two = (sub(0, 1 - gray), sub(1, 1 - top)), (sub(0, gray), sub(1, top))
                low_sums, high_sums = square[s].at[it, run, c, two[0]], square[s].at[it, run, c, two[1]]
                cs["low_three"] = made(6, low_sums, low_sums, y_near)
                cs["high_three"] = made(7, high_sums, high_sums, y_far)
            else:
                one = two = (low, high)
            cs["low_one"] = made(1, rows(mine, one[0]), rows(first_in, one[0]), y_near)
            cs["high_one"] = made(2, rows(mine, one[1]), rows(first_in, one[1]), y_far)
            cs["low_two"] = made(3, rows(ours, two[0]), rows(second_in, two[0]), y_far)
            cs["high_two"] = made(4, rows(ours, two[1]), rows(second_in, two[1]), y_near)
            cs["kept"] = two
            cs["moved"] = first_in[s].at[it, run, low] if three_steps else first_in[s].at[it, run]
            cs["sems"] = [g_recv.at[it, unit_sems[g, s] + kind] for kind in range(5)]
            return cs

        units = {(g, s): unit(g, s) for g in range(len(GROUPS)) for s in range(ns)}

        def strips(g):
            first, n = GROUPS[g]
            return range(first, first + n)

        def factors(g):
            first, n = GROUPS[g]
            columns = slice(first * STRIP, (first + n) * STRIP)
            return block_hi[:, columns], block_lo[:, columns]

        def mul(g, *which):
            first, n = GROUPS[g]
            columns = lanes_of(which[0]) if which else slice(0, NX * STRIP)
            got = three(0, factors(g), (panel_hi[:, columns], panel_lo[:, columns]))
            for s in which or range(ns):
                piece = got if which else got[:, lanes_of(s)]
                part[s][it, first : first + n] = piece.reshape(n, NC, SROWS, piece.shape[1])
                go(units[g, s]["core"])

        def s1(g, s):
            cs = units[g, s]
            cs["core"].wait_recv()
            for p in strips(g):
                mine[s][it, p] = part[s][it, p, c] + from_core[s][it, p]
            go(cs["low_one"])
            go(cs["high_one"])

        def s2(g, s):
            cs = units[g, s]
            all_here(cs["moved"], cs["sems"][1])
            for half, kept in zip(("low", "high"), cs["kept"]):
                for p in strips(g):
                    ours[s][it, p, kept] = mine[s][it, p, kept] + first_in[s][it, p, kept]
                go(cs[half + "_two"])

        def s3(g, s):
            cs = units[g, s]
            all_here(cs["moved"], cs["sems"][2])
            for half, kept in zip(("low", "high"), cs["kept"]):
                for p in strips(g):
                    square[s][it, p, c, kept] = ours[s][it, p, kept] + second_in[s][it, p, kept]
                if half + "_three" in cs:
                    go(cs[half + "_three"])
            if "low_three" not in cs:
                go(cs["join"])

        def s4(g, s):
            cs = units[g, s]
            all_here(cs["moved"], cs["sems"][3])
            go(cs["join"])

        def s6(g, *which):
            first, n = GROUPS[g]
            rows = slice(first * STRIP, (first + n) * STRIP)
            todo = which or range(ns)
            if g in MERGED:
                all_here(block_i.at[pl.ds(0, n), pl.ds(0, HALF)], units[g, 0]["sems"][4])
            for s in todo:
                if g not in MERGED:
                    units[g, s]["join"].wait_recv()
                value = square[s][it, first : first + n]
                value = value.reshape(n * STRIP, value.shape[-1])
                if it == 0:
                    f = factor[0:1, 0:1]
                    value = value * (f * f)
                square_hi[rows, lanes_of(s)], square_lo[rows, lanes_of(s)] = split(value)
            columns = lanes_of(which[0]) if which else slice(0, NX * STRIP)
            b = square_hi[rows, columns], square_lo[rows, columns]
            strip_columns = slice(first * STRIP, (first + n) * STRIP)
            slots = [slot for s in todo for slot in SETS[s]]
            parts = 2 if len(slots) <= 2 else 1
            for part_rows in (slice(k * ROWS // parts, (k + 1) * ROWS // parts) for k in range(parts)):
                a = block_hi[part_rows, strip_columns], block_lo[part_rows, strip_columns]
                got = three(1, a, b)
                for k, slot in enumerate(slots):
                    piece = got[:, k * STRIP : (k + 1) * STRIP]
                    if first == 0:
                        cube[it, slot, part_rows] = piece
                    else:
                        cube[it, slot, part_rows] += piece

        def reduce_copies(r):
            upper, lower = pl.ds(r * PIECE, PIECE), pl.ds(HALF + r * PIECE, PIECE)

            def made(k, slot, rows, dst, peer):
                return copy(cube_i.at[slot, rows], dst, r_send.at[it], r_recv.at[it, r, k // 2], peer)

            return dict(
                chain_up=made(0, 2, upper, x_chain.at[it, r, 0], up_x),
                chain_down=made(1, 2, lower, x_chain.at[it, r, 1], down_x),
                near_down=made(2, 3, upper, x_chain.at[it, r, 2], down_x),
                near_up=made(3, 1, lower, x_chain.at[it, r, 3], up_x),
                end_up=made(4, 1, upper, x_ended.at[it, r, 0], up_x),
                end_down=made(5, 3, lower, x_ended.at[it, r, 1], down_x),
                rows=(upper, lower),
            )

        reduces = [reduce_copies(r) for r in range(2)]

        def rc(r):
            go(reduces[r]["chain_up"])
            go(reduces[r]["chain_down"])

        def rn(r):
            go(reduces[r]["near_up"])
            go(reduces[r]["near_down"])

        def re(r):
            cs = reduces[r]
            all_here(block_i.at[0, pair_rows], r_recv.at[it, r, 0])
            for k, (slot, way) in enumerate(((1, "up"), (3, "down"))):
                cube[it, slot, cs["rows"][k]] += x_chain[it, r, k]
                go(cs["end_" + way])

        def fin(r):
            cs = reduces[r]
            all_here(block_i.at[0, pair_rows], r_recv.at[it, r, 1])
            all_here(block_i.at[0, pair_rows], r_recv.at[it, r, 2])
            for k in range(2):
                rows = cs["rows"][k]
                product = cube[it, 0, rows] + (x_ended[it, r, k] + x_chain[it, r, 2 + k])
                value = block[it, 0, rows]
                if it == 0:
                    f = factor[0:1, 0:1]
                    new = (1.5 * f) * value - (0.5 * f) * product
                else:
                    new = 1.5 * value - 0.5 * product
                if it == ITERS - 1:
                    o_ref[rows] = new
                else:
                    block[it + 1, 0, rows] = new

        sy, sz = {}, {}
        if it == 0:
            for k, peer in enumerate(y_peers, 1):
                sy[k] = copy(sums_y.at[0], sums_y.at[k], s_send.at[0], s_recv.at[0], peer)
            for k, peer in enumerate(z_peers, 1):
                sz[k] = copy(sums_z.at[0], sums_z.at[k], s_send.at[1], s_recv.at[1], peer)

        def sums1():
            tile = jnp.zeros((8, 128), F32)
            for v in (block[it, 0], panel[it, 1], panel[it, 2], panel[it, 3]):
                v = v.reshape(ROWS // 8, 8, STRIP)
                tile = tile + jnp.sum(v * v, axis=0)
            sums_y[0] = tile
            for made in sy.values():
                go(made)

        def sums2():
            all_here(sums_y.at[pl.ds(1, NY * NC - 1)], s_recv.at[0])
            sums_z[0] = jnp.sum(sums_y[...], axis=0)
            for made in sz.values():
                go(made)

        def sums3():
            all_here(sums_z.at[pl.ds(1, NZ - 1)], s_recv.at[1])
            total = jnp.sum(jnp.sum(sums_z[...], axis=0), keepdims=True)
            factor[...] = jnp.broadcast_to(jnp.sqrt(N / total), factor.shape)

        work = dict(
            own=own, zz=zz, put=put, xf=xf, xnear=xnear, xlast=xlast, mul=mul, s1=s1, s2=s2, s3=s3, s4=s4, s6=s6,
            rc=rc, rn=rn, re=re, fin=fin, sums1=sums1, sums2=sums2, sums3=sums3,
        )
        for name, *args in ORDER[it]:
            with jax.named_scope("_".join([f"i{it}", name, *map(str, args)])):
                work[name](*args)

    for it in range(ITERS):
        iteration(it)
    with jax.named_scope("sent"):
        slow = sum(LANES[s][1] * n for g, (_, n) in enumerate(GROUPS) for s in range(ns) if g * ns + s < THREE_STEPS)
        fast, slow = (NX * NZ - slow) // NX, slow // NX
        for it in range(ITERS):
            all_sent(block.at[it, pl.ds(0, NZ - 1)], z_send.at[it])
            all_sent(block.at[it, pl.ds(0, NX - 1)], x_send.at[it])
            all_sent(block.at[it, pl.ds(0, NX - 1)], r_send.at[it])
            all_sent(block.at[it], g_send.at[it, 0])
            all_sent(block.at[it, pl.ds(0, slow), pl.ds(0, HALF)], g_send.at[it, 1])
            all_sent(block.at[it, pl.ds(0, slow), pl.ds(0, PIECE)], g_send.at[it, 2])
            all_sent(block.at[it, pl.ds(0, fast)], g_send.at[it, 3])
        all_sent(sums_y.at[pl.ds(1, NY * NC - 1)], s_send.at[0])
        all_sent(sums_z.at[pl.ds(1, NZ - 1)], s_send.at[1])


def shards(matrix):
    dma = pltpu.SemaphoreType.DMA
    wide = NX * STRIP
    widths = [n * STRIP for _, n in LANES]

    def per_set(*shape):
        return [pltpu.VMEM((ITERS, NZ, *shape, width), F32) for width in widths]

    return pl.pallas_call(
        kernel,
        out_shape=pltpu.VMEM((ROWS, STRIP), F32),
        in_specs=[pl.BlockSpec(memory_space=pltpu.HBM)],
        out_specs=pl.BlockSpec(memory_space=pltpu.VMEM),
        scratch_shapes=[
            pltpu.VMEM((ITERS, NZ, ROWS, STRIP), F32),
            pltpu.VMEM((ITERS, NX, ROWS, STRIP), F32),
            pltpu.VMEM((ROWS, NZ * STRIP), BF),
            pltpu.VMEM((ROWS, NZ * STRIP), BF),
            pltpu.VMEM((ROWS, wide), BF),
            pltpu.VMEM((ROWS, wide), BF),
            pltpu.VMEM((NZ * STRIP, wide), BF),
            pltpu.VMEM((NZ * STRIP, wide), BF),
            *per_set(NC, SROWS),
            *per_set(SROWS),
            *per_set(SROWS),
            *per_set(SROWS),
            *per_set(SROWS),
            *per_set(SROWS),
            *per_set(NC, SROWS),
            pltpu.VMEM((ITERS, NX, ROWS, STRIP), F32),
            pltpu.VMEM((ITERS, 2, 4, PIECE, STRIP), F32),
            pltpu.VMEM((ITERS, 2, 2, PIECE, STRIP), F32),
            pltpu.VMEM((8, 128), F32),
            pltpu.VMEM((NY * NC, 8, 128), F32),
            pltpu.VMEM((NZ, 8, 128), F32),
            dma((ITERS,)),
            dma((ITERS, 4, PIECES)),
            dma((ITERS,)),
            dma((ITERS, 4)),
            dma((ITERS,)),
            dma((ITERS, 2, 3)),
            dma((ITERS, 4)),
            dma((ITERS, 5 * len(GROUPS) * len(SETS))),
            dma((2,)),
            dma((2,)),
            dma((3,)),
        ],
        compiler_params=pltpu.CompilerParams(
            collective_id=0, has_side_effects=True, vmem_limit_bytes=56 * 1024 * 1024
        ),
    )(matrix)


def solution(mesh):
    grid = Mesh(mesh.devices.reshape(NY, NC, NX, NZ), ("y", "c", "x", "z"))
    spec = P(("y", "c"), ("x", "z"))
    return jax.shard_map(shards, mesh=grid, in_specs=(spec,), out_specs=spec, check_vma=False)
```

```python
import jax
import jax.numpy as jnp
from jax import lax
from jax.experimental import pallas as pl
from jax.experimental.pallas import tpu as pltpu
from jax.sharding import Mesh
from jax.sharding import PartitionSpec as P

N = 4096
ITERS = 2
NY, NC, NX, NZ = 4, 2, 4, 8
ROWS = N // (NY * NC)
STRIP = N // (NX * NZ)
HALF = ROWS // 2
PIECES = 4
PIECE = ROWS // PIECES
SROWS = STRIP // NC
SHALF = SROWS // 2
SQUARTER = SROWS // 4
GROUPS = ((0, 1), (1, 2), (3, 2), (5, 2), (7, 1))
SETS = ((2,), (1, 3), (0,))
LANES = ((0, 1), (1, 2), (3, 1))
BF = jnp.bfloat16
F32 = jnp.float32
MERGED = (0,)
THREE_STEPS = 12
ORDER = (
    (
        ("own", 0), ("own", 1), ("put", 0), ("mul", 0, 2), ("s1", 0, 2), ("zz", 0, 0), ("xf", 0), ("s2", 0, 2),
        ("zz", 0, 1), ("zz", 0, 2), ("xf", 1), ("s3", 0, 2), ("zz", 0, 3), ("put", 1), ("put", 2), ("mul", 1, 2),
        ("xnear",), ("mul", 1, 1), ("mul", 0, 1), ("zz", 1, 0), ("s1", 1, 2), ("s4", 0, 2), ("s1", 1, 1),
        ("zz", 1, 1), ("s1", 0, 1), ("xlast",), ("sums1",), ("mul", 0, 0), ("mul", 1, 0), ("zz", 1, 2),
        ("s1", 0, 0), ("s2", 1, 2), ("s1", 1, 0), ("zz", 1, 3), ("put", 3), ("put", 4), ("mul", 2), ("s2", 1, 1),
        ("s2", 0, 1), ("zz", 2, 0), ("sums2",), ("s2", 0, 0), ("s1", 2, 0), ("s1", 2, 1), ("s1", 2, 2),
        ("s3", 1, 2), ("zz", 2, 1), ("s2", 1, 0), ("zz", 2, 2), ("s3", 1, 1), ("s3", 0, 1), ("s3", 0, 0),
        ("s2", 2, 0), ("zz", 2, 3), ("put", 5), ("put", 6), ("mul", 3), ("s2", 2, 1), ("s2", 2, 2), ("s4", 1, 2),
        ("s3", 1, 0), ("s1", 3, 0), ("s4", 1, 1), ("sums3",), ("s4", 0, 1), ("s1", 3, 1), ("s1", 3, 2),
        ("s4", 0, 0), ("put", 7), ("mul", 4), ("s3", 2, 0), ("s6", 0), ("s3", 2, 1), ("s6", 1, 1), ("s6", 1, 2),
        ("s2", 3, 0), ("s4", 1, 0), ("s1", 4, 0), ("s1", 4, 2), ("s3", 2, 2), ("s1", 4, 1), ("s2", 3, 1),
        ("s2", 3, 2), ("s6", 1, 0), ("s4", 2, 0), ("s4", 2, 1), ("s3", 3, 0), ("s6", 2, 0), ("s2", 4, 0),
        ("s2", 4, 2), ("s6", 2, 1), ("s4", 2, 2), ("s2", 4, 1), ("s3", 3, 1), ("s6", 2, 2), ("s3", 3, 2),
        ("s4", 3, 0), ("s3", 4, 0), ("s3", 4, 2), ("s6", 3, 0), ("s6", 4, 0), ("rc", 1), ("rc", 0), ("s3", 4, 1),
        ("s4", 3, 1), ("s4", 3, 2), ("s6", 3, 1), ("s6", 4, 1), ("rn", 0), ("s6", 3, 2), ("s6", 4, 2), ("rn", 1),
        ("re", 1), ("re", 0), ("fin", 1), ("fin", 0),
    ),
    (
        ("own", 1), ("put", 0), ("mul", 0, 2), ("own", 0), ("s1", 0, 2), ("zz", 0, 2), ("xf", 1), ("zz", 0, 3),
        ("s2", 0, 2), ("zz", 0, 0), ("xf", 0), ("zz", 0, 1), ("put", 1), ("put", 2), ("mul", 1, 2), ("xnear",),
        ("mul", 0, 1), ("s3", 0, 2), ("mul", 1, 1), ("zz", 1, 2), ("s1", 1, 2), ("s1", 0, 1), ("zz", 1, 3),
        ("s1", 1, 1), ("xlast",), ("mul", 0, 0), ("mul", 1, 0), ("s4", 0, 2), ("zz", 1, 0), ("s1", 0, 0),
        ("s2", 1, 2), ("s1", 1, 0), ("s2", 0, 1), ("zz", 1, 1), ("put", 4), ("put", 3), ("mul", 2), ("s2", 1, 1),
        ("zz", 2, 2), ("s2", 0, 0), ("s1", 2, 0), ("s1", 2, 1), ("s1", 2, 2), ("s3", 1, 2), ("zz", 2, 3),
        ("s2", 1, 0), ("s3", 0, 1), ("zz", 2, 0), ("s3", 1, 1), ("s3", 0, 0), ("s2", 2, 0), ("zz", 2, 1),
        ("put", 6), ("put", 5), ("mul", 3), ("s2", 2, 1), ("s2", 2, 2), ("s4", 1, 2), ("s3", 1, 0), ("s4", 0, 1),
        ("s1", 3, 0), ("s1", 3, 1), ("s1", 3, 2), ("s4", 1, 1), ("s4", 0, 0), ("put", 7), ("mul", 4), ("s3", 2, 0),
        ("s6", 0), ("s3", 2, 1), ("s6", 1, 1), ("s6", 1, 2), ("s4", 1, 0), ("s3", 2, 2), ("s2", 3, 0), ("s1", 4, 0),
        ("s1", 4, 2), ("s1", 4, 1), ("s2", 3, 1), ("s2", 3, 2), ("s6", 1, 0), ("s4", 2, 0), ("s4", 2, 1),
        ("s4", 2, 2), ("s6", 2, 0), ("s3", 3, 0), ("s2", 4, 0), ("s6", 2, 1), ("s2", 4, 2), ("s6", 2, 2),
        ("s2", 4, 1), ("s3", 3, 1), ("s3", 3, 2), ("s4", 3, 0), ("s3", 4, 0), ("s3", 4, 2), ("s6", 3, 0),
        ("s6", 4, 0), ("rc", 0), ("rc", 1), ("s3", 4, 1), ("s4", 3, 1), ("s4", 3, 2), ("s6", 3, 1), ("s6", 4, 1),
        ("rn", 1), ("rn", 0), ("s6", 3, 2), ("s6", 4, 2), ("re", 0), ("re", 1), ("fin", 0), ("fin", 1),
    ),
)


def split(value):
    high = value.astype(BF)
    return high, (value - high.astype(F32)).astype(BF)


def three(dim, a, b):
    a = jnp.concatenate([a[0], a[1], a[0]], axis=dim)
    b = jnp.concatenate([b[0], b[0], b[1]], axis=0)
    return lax.dot_general(a, b, (((dim,), (0,)), ((), ())), preferred_element_type=F32)


def lanes_of(s):
    first, n = LANES[s]
    return slice(first * STRIP, (first + n) * STRIP)


def kernel(m_ref, o_ref, block, panel, block_hi, block_lo, panel_hi, panel_lo, square_hi, square_lo, *refs):
    ns = len(SETS)
    part, from_core, mine, first_in, ours, second_in, square = (refs[k * ns : (k + 1) * ns] for k in range(7))
    (
        cube, x_chain, x_ended, factor, sums_y, sums_z,
        z_send, z_recv, x_send, x_recv, r_send, r_recv, g_send, g_recv, s_send, s_recv, local_sem,
    ) = refs[7 * ns :]
    y, c, x, z = (lax.axis_index(name) for name in ("y", "c", "x", "z"))

    def turn(name, here, by, size):
        return {name: lax.rem(here + by, size)}

    up_z, down_z = turn("z", z, 1, NZ), turn("z", z, NZ - 1, NZ)
    up_x, down_x = turn("x", x, 1, NX), turn("x", x, NX - 1, NX)
    odd = lax.rem(y, 2)
    y_near, y_far = turn("y", y, NY + 1 - 2 * odd, NY), turn("y", y, NY - 1 + 2 * odd, NY)
    other_core = {"c": 1 - c}
    z_peers = [turn("z", z, d, NZ) for d in range(1, NZ)]
    y_peers = [{"y": lax.rem(y + d, NY), "c": lax.rem(c + e, NC)} for d in range(NY) for e in range(NC)][1:]

    barrier = pltpu.get_barrier_semaphore()
    peers = [up_x, down_x, up_z, down_z, y_near, y_far, other_core]
    for peer in peers:
        pl.semaphore_signal(barrier, inc=1, device_id=peer, device_id_type=pl.DeviceIdType.MESH)
    fetch = pltpu.make_async_copy(m_ref, block.at[0, 0], local_sem.at[0])
    fetch.start()
    with jax.named_scope("fetch"):
        fetch.wait()
    with jax.named_scope("barrier"):
        pl.semaphore_wait(barrier, len(peers))

    def copy(src, dst, send, recv, peer):
        return pltpu.make_async_remote_copy(
            src_ref=src, dst_ref=dst, send_sem=send, recv_sem=recv,
            device_id=peer, device_id_type=pl.DeviceIdType.MESH,
        )

    def go(made):
        made.start()

    def all_sent(ref, sem):
        copy(ref, ref, sem, local_sem.at[2], up_x).wait_send()

    def all_here(ref, sem):
        copy(ref, ref, local_sem.at[2], sem, up_x).wait_recv()

    low, high = pl.ds(0, SHALF), pl.ds(SHALF, SHALF)
    gray, top = lax.rem(lax.div(y + 1, 2), 2), lax.div(y, 2)

    def sub(half, which):
        return pl.ds(pl.multiple_of(half * SHALF + which * SQUARTER, SQUARTER), SQUARTER)


    def iteration(it):
        block_i, panel_i, cube_i = block.at[it], panel.at[it], cube.at[it]

        def piece_of(q):
            return pl.ds(q * PIECE, PIECE)

        def z_copy(src, dst, q, pair, i, peer):
            return copy(
                block_i.at[src, piece_of(q)], block_i.at[dst, piece_of(q)], z_send.at[it], z_recv.at[it, pair, i], peer
            )

        up_order, down_order = (0, 2, 1, 3), (2, 0, 3, 1)
        ups, downs = {}, {}
        for pair in range(3):
            for i in range(PIECES):
                q, d = up_order[i], down_order[i]
                ups[pair, i] = z_copy(max(2 * pair, 0), 2 * pair + 2, q, pair, i, up_z)
                downs[pair, i] = z_copy(max(2 * pair - 1, 0), 2 * pair + 1, d, pair, i, down_z)
        for i in (0, 2):
            ups[3, i] = z_copy(6, 7, up_order[i], 3, 0, up_z)
            downs[3, i] = z_copy(5, 7, down_order[i], 3, 0, down_z)

        def x_copy(src, dst, q, k, peer):
            return copy(src.at[piece_of(q)], panel_i.at[dst, piece_of(q)], x_send.at[it], x_recv.at[it, k], peer)

        x_up = [x_copy(block_i.at[0], 3, q, (0, 1, 2, 2)[q], up_x) for q in range(PIECES)]
        x_down = [x_copy(block_i.at[0], 1, q, (2, 2, 0, 1)[q], down_x) for q in range(PIECES)]
        x_far = [x_copy(panel_i.at[3 - 2 * (q // 2)], 2, q, 3, (up_x, down_x)[q // 2]) for q in range(PIECES)]
        pair_rows = pl.ds(0, 2 * PIECE)

        def put_panel(slot, value):
            at = {2: 0, 1: 1, 3: 2, 0: 3}[slot]
            columns = slice(at * STRIP, (at + 1) * STRIP)
            panel_hi[:, columns], panel_lo[:, columns] = split(value)

        def own(h):
            for q, d in ((h, 2 + h), (2 + h, h)):
                go(x_up[q])
                go(x_down[d])
                i = up_order.index(q)
                go(ups[0, i])
                go(downs[0, i])

        def zz(pair, i):
            all_here(block_i.at[0, pair_rows], z_recv.at[it, pair, i])
            if (pair + 1, i) in ups:
                go(ups[pair + 1, i])
                go(downs[pair + 1, i])

        def put(pos):
            if pos == 7:
                all_here(block_i.at[0], z_recv.at[it, 3, 0])
            columns = slice(pos * STRIP, (pos + 1) * STRIP)
            value = block[it, pos]
            block_hi[:, columns], block_lo[:, columns] = split(value)
            if pos == 0:
                put_panel(0, value)

        def xf(i):
            all_here(block_i.at[0, pair_rows], x_recv.at[it, i])
            go(x_far[i])
            go(x_far[2 + i])

        def xnear():
            all_here(block_i.at[0], x_recv.at[it, 2])
            put_panel(3, panel[it, 3])
            put_panel(1, panel[it, 1])

        def xlast():
            all_here(block_i.at[0], x_recv.at[it, 3])
            put_panel(2, panel[it, 2])

        unit_sems, count = {}, 0
        for g in range(len(GROUPS)):
            for s in range(ns):
                unit_sems[g, s] = count
                count += 5

        def unit(g, s):
            run = pl.ds(*GROUPS[g])
            every = slice(None)

            three_steps = g * ns + s < THREE_STEPS

            def made(k, src, dst, peer):
                kind = (0, 1, 1, 2, 2, 4, 3, 3)[k]
                to = 0 if kind in (0, 4) else 3 if not three_steps else 2 if kind == 2 else 1
                wide = 0 if kind == 4 and g in MERGED else s
                return copy(src, dst, g_send.at[it, to], g_recv.at[unit_sems[g, wide] + kind], peer)

            def rows(ref, which):
                return ref[s].at[it, run, which]

            sums = square[s].at[it, run, c]
            cs = dict(
                core=made(0, part[s].at[it, run, 1 - c], from_core[s].at[it, run], other_core),
                join=made(5, sums, sums, other_core),
            )
            if three_steps:
                one, two = (sub(0, 1 - gray), sub(1, 1 - top)), (sub(0, gray), sub(1, top))
                low_sums, high_sums = square[s].at[it, run, c, two[0]], square[s].at[it, run, c, two[1]]
                cs["low_three"] = made(6, low_sums, low_sums, y_near)
                cs["high_three"] = made(7, high_sums, high_sums, y_far)
            else:
                one = two = (low, high)
            cs["low_one"] = made(1, rows(mine, one[0]), rows(first_in, one[0]), y_near)
            cs["high_one"] = made(2, rows(mine, one[1]), rows(first_in, one[1]), y_far)
            cs["low_two"] = made(3, rows(ours, two[0]), rows(second_in, two[0]), y_far)
            cs["high_two"] = made(4, rows(ours, two[1]), rows(second_in, two[1]), y_near)
            cs["kept"] = two
            cs["moved"] = first_in[s].at[it, run, low] if three_steps else first_in[s].at[it, run]
            cs["sems"] = [g_recv.at[unit_sems[g, s] + kind] for kind in range(5)]
            return cs

        units = {(g, s): unit(g, s) for g in range(len(GROUPS)) for s in range(ns)}

        def strips(g):
            first, n = GROUPS[g]
            return range(first, first + n)

        def factors(g):
            first, n = GROUPS[g]
            columns = slice(first * STRIP, (first + n) * STRIP)
            return block_hi[:, columns], block_lo[:, columns]

        def mul(g, *which):
            first, n = GROUPS[g]
            columns = lanes_of(which[0]) if which else slice(0, NX * STRIP)
            got = three(0, factors(g), (panel_hi[:, columns], panel_lo[:, columns]))
            for s in which or range(ns):
                piece = got if which else got[:, lanes_of(s)]
                part[s][it, first : first + n] = piece.reshape(n, NC, SROWS, piece.shape[1])
                go(units[g, s]["core"])

        def s1(g, s):
            cs = units[g, s]
            cs["core"].wait_recv()
            for p in strips(g):
                mine[s][it, p] = part[s][it, p, c] + from_core[s][it, p]
            go(cs["low_one"])
            go(cs["high_one"])

        def s2(g, s):
            cs = units[g, s]
            all_here(cs["moved"], cs["sems"][1])
            for half, kept in zip(("low", "high"), cs["kept"]):
                for p in strips(g):
                    ours[s][it, p, kept] = mine[s][it, p, kept] + first_in[s][it, p, kept]
                go(cs[half + "_two"])

        def s3(g, s):
            cs = units[g, s]
            all_here(cs["moved"], cs["sems"][2])
            for half, kept in zip(("low", "high"), cs["kept"]):
                for p in strips(g):
                    square[s][it, p, c, kept] = ours[s][it, p, kept] + second_in[s][it, p, kept]
                if half + "_three" in cs:
                    go(cs[half + "_three"])
            if "low_three" not in cs:
                go(cs["join"])

        def s4(g, s):
            cs = units[g, s]
            all_here(cs["moved"], cs["sems"][3])
            go(cs["join"])

        def s6(g, *which):
            first, n = GROUPS[g]
            rows = slice(first * STRIP, (first + n) * STRIP)
            todo = which or range(ns)
            if g in MERGED:
                all_here(block_i.at[pl.ds(0, n), pl.ds(0, HALF)], units[g, 0]["sems"][4])
            for s in todo:
                if g not in MERGED:
                    units[g, s]["join"].wait_recv()
                value = square[s][it, first : first + n]
                value = value.reshape(n * STRIP, value.shape[-1])
                if it == 0:
                    f = factor[0:1, 0:1]
                    value = value * (f * f)
                square_hi[rows, lanes_of(s)], square_lo[rows, lanes_of(s)] = split(value)
            columns = lanes_of(which[0]) if which else slice(0, NX * STRIP)
            b = square_hi[rows, columns], square_lo[rows, columns]
            strip_columns = slice(first * STRIP, (first + n) * STRIP)
            slots = [slot for s in todo for slot in SETS[s]]
            parts = 2 if len(slots) <= 2 else 1
            for part_rows in (slice(k * ROWS // parts, (k + 1) * ROWS // parts) for k in range(parts)):
                a = block_hi[part_rows, strip_columns], block_lo[part_rows, strip_columns]
                got = three(1, a, b)
                for k, slot in enumerate(slots):
                    piece = got[:, k * STRIP : (k + 1) * STRIP]
                    if first == 0:
                        cube[it, slot, part_rows] = piece
                    else:
                        cube[it, slot, part_rows] += piece

        def reduce_copies(r):
            upper, lower = pl.ds(r * PIECE, PIECE), pl.ds(HALF + r * PIECE, PIECE)

            def made(k, slot, rows, dst, peer):
                return copy(cube_i.at[slot, rows], dst, r_send.at[it], r_recv.at[it, r, k // 2], peer)

            return dict(
                chain_up=made(0, 2, upper, x_chain.at[it, r, 0], up_x),
                chain_down=made(1, 2, lower, x_chain.at[it, r, 1], down_x),
                near_down=made(2, 3, upper, x_chain.at[it, r, 2], down_x),
                near_up=made(3, 1, lower, x_chain.at[it, r, 3], up_x),
                end_up=made(4, 1, upper, x_ended.at[it, r, 0], up_x),
                end_down=made(5, 3, lower, x_ended.at[it, r, 1], down_x),
                rows=(upper, lower),
            )

        reduces = [reduce_copies(r) for r in range(2)]

        def rc(r):
            go(reduces[r]["chain_up"])
            go(reduces[r]["chain_down"])

        def rn(r):
            go(reduces[r]["near_up"])
            go(reduces[r]["near_down"])

        def re(r):
            cs = reduces[r]
            all_here(block_i.at[0, pair_rows], r_recv.at[it, r, 0])
            for k, (slot, way) in enumerate(((1, "up"), (3, "down"))):
                cube[it, slot, cs["rows"][k]] += x_chain[it, r, k]
                go(cs["end_" + way])

        def fin(r):
            cs = reduces[r]
            all_here(block_i.at[0, pair_rows], r_recv.at[it, r, 1])
            all_here(block_i.at[0, pair_rows], r_recv.at[it, r, 2])
            for k in range(2):
                rows = cs["rows"][k]
                product = cube[it, 0, rows] + (x_ended[it, r, k] + x_chain[it, r, 2 + k])
                value = block[it, 0, rows]
                if it == 0:
                    f = factor[0:1, 0:1]
                    new = (1.5 * f) * value - (0.5 * f) * product
                else:
                    new = 1.5 * value - 0.5 * product
                if it == ITERS - 1:
                    o_ref[rows] = new
                else:
                    block[it + 1, 0, rows] = new

        sy, sz = {}, {}
        if it == 0:
            for k, peer in enumerate(y_peers, 1):
                sy[k] = copy(sums_y.at[0], sums_y.at[k], s_send.at[0], s_recv.at[0], peer)
            for k, peer in enumerate(z_peers, 1):
                sz[k] = copy(sums_z.at[0], sums_z.at[k], s_send.at[1], s_recv.at[1], peer)

        def sums1():
            tile = jnp.zeros((8, 128), F32)
            for v in (block[it, 0], panel[it, 1], panel[it, 2], panel[it, 3]):
                v = v.reshape(ROWS // 8, 8, STRIP)
                tile = tile + jnp.sum(v * v, axis=0)
            sums_y[0] = tile
            for made in sy.values():
                go(made)

        def sums2():
            all_here(sums_y.at[pl.ds(1, NY * NC - 1)], s_recv.at[0])
            sums_z[0] = jnp.sum(sums_y[...], axis=0)
            for made in sz.values():
                go(made)

        def sums3():
            all_here(sums_z.at[pl.ds(1, NZ - 1)], s_recv.at[1])
            total = jnp.sum(jnp.sum(sums_z[...], axis=0), keepdims=True)
            factor[...] = jnp.broadcast_to(jnp.sqrt(N / total), factor.shape)

        work = dict(
            own=own, zz=zz, put=put, xf=xf, xnear=xnear, xlast=xlast, mul=mul, s1=s1, s2=s2, s3=s3, s4=s4, s6=s6,
            rc=rc, rn=rn, re=re, fin=fin, sums1=sums1, sums2=sums2, sums3=sums3,
        )
        for name, *args in ORDER[it]:
            with jax.named_scope("_".join([f"i{it}", name, *map(str, args)])):
                work[name](*args)

    for it in range(ITERS):
        iteration(it)
    with jax.named_scope("sent"):
        slow = sum(LANES[s][1] * n for g, (_, n) in enumerate(GROUPS) for s in range(ns) if g * ns + s < THREE_STEPS)
        fast, slow = (NX * NZ - slow) // NX, slow // NX
        for it in range(ITERS):
            all_sent(block.at[it, pl.ds(0, NZ - 1)], z_send.at[it])
            all_sent(block.at[it, pl.ds(0, NX - 1)], x_send.at[it])
            all_sent(block.at[it, pl.ds(0, NX - 1)], r_send.at[it])
            all_sent(block.at[it], g_send.at[it, 0])
            all_sent(block.at[it, pl.ds(0, slow), pl.ds(0, HALF)], g_send.at[it, 1])
            all_sent(block.at[it, pl.ds(0, slow), pl.ds(0, PIECE)], g_send.at[it, 2])
            all_sent(block.at[it, pl.ds(0, fast)], g_send.at[it, 3])
        all_sent(sums_y.at[pl.ds(1, NY * NC - 1)], s_send.at[0])
        all_sent(sums_z.at[pl.ds(1, NZ - 1)], s_send.at[1])


def shards(matrix):
    dma = pltpu.SemaphoreType.DMA
    wide = NX * STRIP
    widths = [n * STRIP for _, n in LANES]

    def per_set(*shape):
        return [pltpu.VMEM((ITERS, NZ, *shape, width), F32) for width in widths]

    return pl.pallas_call(
        kernel,
        out_shape=pltpu.VMEM((ROWS, STRIP), F32),
        in_specs=[pl.BlockSpec(memory_space=pltpu.HBM)],
        out_specs=pl.BlockSpec(memory_space=pltpu.VMEM),
        scratch_shapes=[
            pltpu.VMEM((ITERS, NZ, ROWS, STRIP), F32),
            pltpu.VMEM((ITERS, NX, ROWS, STRIP), F32),
            pltpu.VMEM((ROWS, NZ * STRIP), BF),
            pltpu.VMEM((ROWS, NZ * STRIP), BF),
            pltpu.VMEM((ROWS, wide), BF),
            pltpu.VMEM((ROWS, wide), BF),
            pltpu.VMEM((NZ * STRIP, wide), BF),
            pltpu.VMEM((NZ * STRIP, wide), BF),
            *per_set(NC, SROWS),
            *per_set(SROWS),
            *per_set(SROWS),
            *per_set(SROWS),
            *per_set(SROWS),
            *per_set(SROWS),
            *per_set(NC, SROWS),
            pltpu.VMEM((ITERS, NX, ROWS, STRIP), F32),
            pltpu.VMEM((ITERS, 2, 4, PIECE, STRIP), F32),
            pltpu.VMEM((ITERS, 2, 2, PIECE, STRIP), F32),
            pltpu.VMEM((8, 128), F32),
            pltpu.VMEM((NY * NC, 8, 128), F32),
            pltpu.VMEM((NZ, 8, 128), F32),
            dma((ITERS,)),
            dma((ITERS, 4, PIECES)),
            dma((ITERS,)),
            dma((ITERS, 4)),
            dma((ITERS,)),
            dma((ITERS, 2, 3)),
            dma((ITERS, 4)),
            dma((5 * len(GROUPS) * len(SETS),)),
            dma((2,)),
            dma((2,)),
            dma((3,)),
        ],
        compiler_params=pltpu.CompilerParams(
            collective_id=0, has_side_effects=True, vmem_limit_bytes=56 * 1024 * 1024
        ),
    )(matrix)


def solution(mesh):
    grid = Mesh(mesh.devices.reshape(NY, NC, NX, NZ), ("y", "c", "x", "z"))
    spec = P(("y", "c"), ("x", "z"))
    return jax.shard_map(shards, mesh=grid, in_specs=(spec,), out_specs=spec, check_vma=False)
```

```python
import jax
import jax.numpy as jnp
from jax import lax
from jax.experimental import pallas as pl
from jax.experimental.pallas import tpu as pltpu
from jax.sharding import Mesh
from jax.sharding import PartitionSpec as P

N = 4096
ITERS = 2
NY, NC, NX, NZ = 4, 2, 4, 8
ROWS = N // (NY * NC)
STRIP = N // (NX * NZ)
HALF = ROWS // 2
PIECES = 4
PIECE = ROWS // PIECES
SROWS = STRIP // NC
SHALF = SROWS // 2
SQUARTER = SROWS // 4
GROUPS = ((0, 1), (1, 2), (3, 2), (5, 2), (7, 1))
SETS = ((2,), (1, 3), (0,))
LANES = ((0, 1), (1, 2), (3, 1))
BF = jnp.bfloat16
F32 = jnp.float32
MERGED = (0,)
THREE_STEPS = 12
ORDER = (
    (
        ("own", 0), ("own", 1), ("put", 0), ("mul", 0, 2), ("s1", 0, 2), ("zz", 0, 0), ("xf", 0), ("s2", 0, 2),
        ("zz", 0, 1), ("zz", 0, 2), ("xf", 1), ("s3", 0, 2), ("zz", 0, 3), ("put", 1), ("put", 2), ("mul", 1, 2),
        ("xnear",), ("mul", 1, 1), ("mul", 0, 1), ("zz", 1, 0), ("s1", 1, 2), ("s4", 0, 2), ("s1", 1, 1),
        ("zz", 1, 1), ("s1", 0, 1), ("xlast",), ("sums1",), ("mul", 0, 0), ("mul", 1, 0), ("zz", 1, 2),
        ("s1", 0, 0), ("s2", 1, 2), ("s1", 1, 0), ("zz", 1, 3), ("put", 3), ("put", 4), ("mul", 2), ("s2", 1, 1),
        ("s2", 0, 1), ("zz", 2, 0), ("sums2",), ("s2", 0, 0), ("s1", 2, 0), ("s1", 2, 1), ("s1", 2, 2),
        ("s3", 1, 2), ("zz", 2, 1), ("s2", 1, 0), ("zz", 2, 2), ("s3", 1, 1), ("s3", 0, 1), ("s3", 0, 0),
        ("s2", 2, 0), ("zz", 2, 3), ("put", 5), ("put", 6), ("mul", 3), ("s2", 2, 1), ("s2", 2, 2), ("s4", 1, 2),
        ("s3", 1, 0), ("s1", 3, 0), ("s4", 1, 1), ("sums3",), ("s4", 0, 1), ("s1", 3, 1), ("s1", 3, 2),
        ("s4", 0, 0), ("put", 7), ("mul", 4), ("s3", 2, 0), ("s6", 0), ("s3", 2, 1), ("s6", 1, 1), ("s6", 1, 2),
        ("s2", 3, 0), ("s4", 1, 0), ("s1", 4, 0), ("s1", 4, 2), ("s3", 2, 2), ("s1", 4, 1), ("s2", 3, 1),
        ("s2", 3, 2), ("s6", 1, 0), ("s4", 2, 0), ("s4", 2, 1), ("s3", 3, 0), ("s6", 2, 0), ("s2", 4, 0),
        ("s2", 4, 2), ("s6", 2, 1), ("s4", 2, 2), ("s2", 4, 1), ("s3", 3, 1), ("s6", 2, 2), ("s3", 3, 2),
        ("s4", 3, 0), ("s3", 4, 0), ("s3", 4, 2), ("s6", 3, 0), ("s6", 4, 0), ("rc", 1), ("rc", 0), ("s3", 4, 1),
        ("s4", 3, 1), ("s4", 3, 2), ("s6", 3, 1), ("s6", 4, 1), ("rn", 0), ("s6", 3, 2), ("s6", 4, 2), ("rn", 1),
        ("re", 1), ("re", 0), ("fin", 1), ("fin", 0),
    ),
    (
        ("own", 1), ("put", 0), ("mul", 0, 2), ("own", 0), ("s1", 0, 2), ("zz", 0, 2), ("xf", 1), ("zz", 0, 3),
        ("s2", 0, 2), ("zz", 0, 0), ("xf", 0), ("zz", 0, 1), ("put", 1), ("put", 2), ("mul", 1, 2), ("xnear",),
        ("mul", 0, 1), ("s3", 0, 2), ("mul", 1, 1), ("zz", 1, 2), ("s1", 1, 2), ("s1", 0, 1), ("zz", 1, 3),
        ("s1", 1, 1), ("xlast",), ("mul", 0, 0), ("mul", 1, 0), ("s4", 0, 2), ("zz", 1, 0), ("s1", 0, 0),
        ("s2", 1, 2), ("s1", 1, 0), ("s2", 0, 1), ("zz", 1, 1), ("put", 4), ("put", 3), ("mul", 2), ("s2", 1, 1),
        ("zz", 2, 2), ("s2", 0, 0), ("s1", 2, 0), ("s1", 2, 1), ("s1", 2, 2), ("s3", 1, 2), ("zz", 2, 3),
        ("s2", 1, 0), ("s3", 0, 1), ("zz", 2, 0), ("s3", 1, 1), ("s3", 0, 0), ("s2", 2, 0), ("zz", 2, 1),
        ("put", 6), ("put", 5), ("mul", 3), ("s2", 2, 1), ("s2", 2, 2), ("s4", 1, 2), ("s3", 1, 0), ("s4", 0, 1),
        ("s1", 3, 0), ("s1", 3, 1), ("s1", 3, 2), ("s4", 1, 1), ("s4", 0, 0), ("put", 7), ("mul", 4), ("s3", 2, 0),
        ("s6", 0), ("s3", 2, 1), ("s6", 1, 1), ("s6", 1, 2), ("s4", 1, 0), ("s3", 2, 2), ("s2", 3, 0), ("s1", 4, 0),
        ("s1", 4, 2), ("s1", 4, 1), ("s2", 3, 1), ("s2", 3, 2), ("s6", 1, 0), ("s4", 2, 0), ("s4", 2, 1),
        ("s4", 2, 2), ("s6", 2, 0), ("s3", 3, 0), ("s2", 4, 0), ("s6", 2, 1), ("s2", 4, 2), ("s6", 2, 2),
        ("s2", 4, 1), ("s3", 3, 1), ("s3", 3, 2), ("s4", 3, 0), ("s3", 4, 0), ("s3", 4, 2), ("s6", 3, 0),
        ("s6", 4, 0), ("rc", 0), ("rc", 1), ("s3", 4, 1), ("s4", 3, 1), ("s4", 3, 2), ("s6", 3, 1), ("s6", 4, 1),
        ("rn", 1), ("rn", 0), ("s6", 3, 2), ("s6", 4, 2), ("re", 0), ("re", 1), ("fin", 0), ("fin", 1),
    ),
)


def split(value):
    high = value.astype(BF)
    return high, (value - high.astype(F32)).astype(BF)


def three(dim, a, b):
    a = jnp.concatenate([a[0], a[1], a[0]], axis=dim)
    b = jnp.concatenate([b[0], b[0], b[1]], axis=0)
    return lax.dot_general(a, b, (((dim,), (0,)), ((), ())), preferred_element_type=F32)


def lanes_of(s):
    first, n = LANES[s]
    return slice(first * STRIP, (first + n) * STRIP)


def kernel(m_ref, o_ref, block, panel, block_hi, block_lo, panel_hi, panel_lo, square_hi, square_lo, *refs):
    ns = len(SETS)
    part, from_core, mine, first_in, ours, second_in, square = (refs[k * ns : (k + 1) * ns] for k in range(7))
    (
        cube, x_chain, x_ended, factor, sums_y, sums_z,
        z_send, z_recv, x_send, x_recv, r_send, r_recv, g_send, g_recv, s_send, s_recv, local_sem,
    ) = refs[7 * ns :]
    y, c, x, z = (lax.axis_index(name) for name in ("y", "c", "x", "z"))

    def turn(name, here, by, size):
        return {name: lax.rem(here + by, size)}

    up_z, down_z = turn("z", z, 1, NZ), turn("z", z, NZ - 1, NZ)
    up_x, down_x = turn("x", x, 1, NX), turn("x", x, NX - 1, NX)
    odd = lax.rem(y, 2)
    y_near, y_far = turn("y", y, NY + 1 - 2 * odd, NY), turn("y", y, NY - 1 + 2 * odd, NY)
    other_core = {"c": 1 - c}
    z_peers = [turn("z", z, d, NZ) for d in range(1, NZ)]
    y_peers = [{"y": lax.rem(y + d, NY), "c": lax.rem(c + e, NC)} for d in range(NY) for e in range(NC)][1:]

    barrier = pltpu.get_barrier_semaphore()
    peers = [up_x, down_x, up_z, down_z, y_near, y_far, other_core]
    for peer in peers:
        pl.semaphore_signal(barrier, inc=1, device_id=peer, device_id_type=pl.DeviceIdType.MESH)
    fetch = pltpu.make_async_copy(m_ref, block.at[0, 0], local_sem.at[0])
    fetch.start()
    with jax.named_scope("fetch"):
        fetch.wait()
    with jax.named_scope("barrier"):
        pl.semaphore_wait(barrier, len(peers))

    def copy(src, dst, send, recv, peer):
        return pltpu.make_async_remote_copy(
            src_ref=src, dst_ref=dst, send_sem=send, recv_sem=recv,
            device_id=peer, device_id_type=pl.DeviceIdType.MESH,
        )

    def go(made):
        made.start()

    def all_sent(ref, sem):
        copy(ref, ref, sem, local_sem.at[1], up_x).wait_send()

    def all_here(ref, sem):
        copy(ref, ref, local_sem.at[1], sem, up_x).wait_recv()

    low, high = pl.ds(0, SHALF), pl.ds(SHALF, SHALF)
    gray, top = lax.rem(lax.div(y + 1, 2), 2), lax.div(y, 2)

    def sub(half, which):
        return pl.ds(pl.multiple_of(half * SHALF + which * SQUARTER, SQUARTER), SQUARTER)


    def iteration(it):
        block_i, panel_i, cube_i = block.at[it], panel.at[it], cube.at[it]

        def piece_of(q):
            return pl.ds(q * PIECE, PIECE)

        def z_copy(src, dst, q, pair, i, peer):
            return copy(
                block_i.at[src, piece_of(q)], block_i.at[dst, piece_of(q)], z_send.at[it], z_recv.at[it, PIECES * pair + i], peer
            )

        up_order, down_order = (0, 2, 1, 3), (2, 0, 3, 1)
        ups, downs = {}, {}
        for pair in range(3):
            for i in range(PIECES):
                q, d = up_order[i], down_order[i]
                ups[pair, i] = z_copy(max(2 * pair, 0), 2 * pair + 2, q, pair, i, up_z)
                downs[pair, i] = z_copy(max(2 * pair - 1, 0), 2 * pair + 1, d, pair, i, down_z)
        for i in (0, 2):
            ups[3, i] = z_copy(6, 7, up_order[i], 3, 0, up_z)
            downs[3, i] = z_copy(5, 7, down_order[i], 3, 0, down_z)

        def x_copy(src, dst, q, k, peer):
            return copy(src.at[piece_of(q)], panel_i.at[dst, piece_of(q)], x_send.at[it], x_recv.at[k], peer)

        x_up = [x_copy(block_i.at[0], 3, q, (0, 1, 2, 2)[q], up_x) for q in range(PIECES)]
        x_down = [x_copy(block_i.at[0], 1, q, (2, 2, 0, 1)[q], down_x) for q in range(PIECES)]
        x_far = [x_copy(panel_i.at[3 - 2 * (q // 2)], 2, q, 3, (up_x, down_x)[q // 2]) for q in range(PIECES)]
        pair_rows = pl.ds(0, 2 * PIECE)

        def put_panel(slot, value):
            at = {2: 0, 1: 1, 3: 2, 0: 3}[slot]
            columns = slice(at * STRIP, (at + 1) * STRIP)
            panel_hi[:, columns], panel_lo[:, columns] = split(value)

        def own(h):
            for q, d in ((h, 2 + h), (2 + h, h)):
                go(x_up[q])
                go(x_down[d])
                i = up_order.index(q)
                go(ups[0, i])
                go(downs[0, i])

        def zz(pair, i):
            all_here(block_i.at[0, pair_rows], z_recv.at[it, PIECES * pair + i])
            if (pair + 1, i) in ups:
                go(ups[pair + 1, i])
                go(downs[pair + 1, i])

        def put(pos):
            if pos == 7:
                all_here(block_i.at[0], z_recv.at[it, 3 * PIECES])
            columns = slice(pos * STRIP, (pos + 1) * STRIP)
            value = block[it, pos]
            block_hi[:, columns], block_lo[:, columns] = split(value)
            if pos == 0:
                put_panel(0, value)

        def xf(i):
            all_here(block_i.at[0, pair_rows], x_recv.at[i])
            go(x_far[i])
            go(x_far[2 + i])

        def xnear():
            all_here(block_i.at[0], x_recv.at[2])
            put_panel(3, panel[it, 3])
            put_panel(1, panel[it, 1])

        def xlast():
            all_here(block_i.at[0], x_recv.at[3])
            put_panel(2, panel[it, 2])

        unit_sems, count = {}, 0
        for g in range(len(GROUPS)):
            for s in range(ns):
                unit_sems[g, s] = count
                count += 4

        def unit(g, s):
            run = pl.ds(*GROUPS[g])
            every = slice(None)

            three_steps = g * ns + s < THREE_STEPS

            def made(k, src, dst, peer):
                kind = (0, 1, 1, 2, 2, 3, 1, 1)[k]
                to = 0 if kind in (0, 3) else 3 if not three_steps else 2 if kind == 2 else 1
                wide = 0 if kind == 3 and g in MERGED else s
                return copy(src, dst, g_send.at[it, to], g_recv.at[unit_sems[g, wide] + kind], peer)

            def rows(ref, which):
                return ref[s].at[it, run, which]

            sums = square[s].at[it, run, c]
            cs = dict(
                core=made(0, part[s].at[it, run, 1 - c], from_core[s].at[it, run], other_core),
                join=made(5, sums, sums, other_core),
            )
            if three_steps:
                one, two = (sub(0, 1 - gray), sub(1, 1 - top)), (sub(0, gray), sub(1, top))
                low_sums, high_sums = square[s].at[it, run, c, two[0]], square[s].at[it, run, c, two[1]]
                cs["low_three"] = made(6, low_sums, low_sums, y_near)
                cs["high_three"] = made(7, high_sums, high_sums, y_far)
            else:
                one = two = (low, high)
            cs["low_one"] = made(1, rows(mine, one[0]), rows(first_in, one[0]), y_near)
            cs["high_one"] = made(2, rows(mine, one[1]), rows(first_in, one[1]), y_far)
            cs["low_two"] = made(3, rows(ours, two[0]), rows(second_in, two[0]), y_far)
            cs["high_two"] = made(4, rows(ours, two[1]), rows(second_in, two[1]), y_near)
            cs["kept"] = two
            cs["moved"] = first_in[s].at[it, run, low] if three_steps else first_in[s].at[it, run]
            cs["sems"] = [g_recv.at[unit_sems[g, s] + kind] for kind in range(4)]
            return cs

        units = {(g, s): unit(g, s) for g in range(len(GROUPS)) for s in range(ns)}

        def strips(g):
            first, n = GROUPS[g]
            return range(first, first + n)

        def factors(g):
            first, n = GROUPS[g]
            columns = slice(first * STRIP, (first + n) * STRIP)
            return block_hi[:, columns], block_lo[:, columns]

        def mul(g, *which):
            first, n = GROUPS[g]
            columns = lanes_of(which[0]) if which else slice(0, NX * STRIP)
            got = three(0, factors(g), (panel_hi[:, columns], panel_lo[:, columns]))
            for s in which or range(ns):
                piece = got if which else got[:, lanes_of(s)]
                part[s][it, first : first + n] = piece.reshape(n, NC, SROWS, piece.shape[1])
                go(units[g, s]["core"])

        def s1(g, s):
            cs = units[g, s]
            cs["core"].wait_recv()
            for p in strips(g):
                mine[s][it, p] = part[s][it, p, c] + from_core[s][it, p]
            go(cs["low_one"])
            go(cs["high_one"])

        def s2(g, s):
            cs = units[g, s]
            all_here(cs["moved"], cs["sems"][1])
            for half, kept in zip(("low", "high"), cs["kept"]):
                for p in strips(g):
                    ours[s][it, p, kept] = mine[s][it, p, kept] + first_in[s][it, p, kept]
                go(cs[half + "_two"])

        def s3(g, s):
            cs = units[g, s]
            all_here(cs["moved"], cs["sems"][2])
            for half, kept in zip(("low", "high"), cs["kept"]):
                for p in strips(g):
                    square[s][it, p, c, kept] = ours[s][it, p, kept] + second_in[s][it, p, kept]
                if half + "_three" in cs:
                    go(cs[half + "_three"])
            if "low_three" not in cs:
                go(cs["join"])

        def s4(g, s):
            cs = units[g, s]
            all_here(cs["moved"], cs["sems"][1])
            go(cs["join"])

        def s6(g, *which):
            first, n = GROUPS[g]
            rows = slice(first * STRIP, (first + n) * STRIP)
            todo = which or range(ns)
            if g in MERGED:
                all_here(block_i.at[pl.ds(0, n), pl.ds(0, HALF)], units[g, 0]["sems"][3])
            for s in todo:
                if g not in MERGED:
                    units[g, s]["join"].wait_recv()
                value = square[s][it, first : first + n]
                value = value.reshape(n * STRIP, value.shape[-1])
                if it == 0:
                    f = factor[0:1, 0:1]
                    value = value * (f * f)
                square_hi[rows, lanes_of(s)], square_lo[rows, lanes_of(s)] = split(value)
            columns = lanes_of(which[0]) if which else slice(0, NX * STRIP)
            b = square_hi[rows, columns], square_lo[rows, columns]
            strip_columns = slice(first * STRIP, (first + n) * STRIP)
            slots = [slot for s in todo for slot in SETS[s]]
            parts = 2 if len(slots) <= 2 else 1
            for part_rows in (slice(k * ROWS // parts, (k + 1) * ROWS // parts) for k in range(parts)):
                a = block_hi[part_rows, strip_columns], block_lo[part_rows, strip_columns]
                got = three(1, a, b)
                for k, slot in enumerate(slots):
                    piece = got[:, k * STRIP : (k + 1) * STRIP]
                    if first == 0:
                        cube[it, slot, part_rows] = piece
                    else:
                        cube[it, slot, part_rows] += piece

        def reduce_copies(r):
            upper, lower = pl.ds(r * PIECE, PIECE), pl.ds(HALF + r * PIECE, PIECE)

            def made(k, slot, rows, dst, peer):
                return copy(cube_i.at[slot, rows], dst, r_send.at[it], r_recv.at[r, k // 2], peer)

            return dict(
                chain_up=made(0, 2, upper, x_chain.at[it, r, 0], up_x),
                chain_down=made(1, 2, lower, x_chain.at[it, r, 1], down_x),
                near_down=made(2, 3, upper, x_chain.at[it, r, 2], down_x),
                near_up=made(3, 1, lower, x_chain.at[it, r, 3], up_x),
                end_up=made(4, 1, upper, x_ended.at[it, r, 0], up_x),
                end_down=made(5, 3, lower, x_ended.at[it, r, 1], down_x),
                rows=(upper, lower),
            )

        reduces = [reduce_copies(r) for r in range(2)]

        def rc(r):
            go(reduces[r]["chain_up"])
            go(reduces[r]["chain_down"])

        def rn(r):
            go(reduces[r]["near_up"])
            go(reduces[r]["near_down"])

        def re(r):
            cs = reduces[r]
            all_here(block_i.at[0, pair_rows], r_recv.at[r, 0])
            for k, (slot, way) in enumerate(((1, "up"), (3, "down"))):
                cube[it, slot, cs["rows"][k]] += x_chain[it, r, k]
                go(cs["end_" + way])

        def fin(r):
            cs = reduces[r]
            all_here(block_i.at[0, pair_rows], r_recv.at[r, 1])
            all_here(block_i.at[0, pair_rows], r_recv.at[r, 2])
            for k in range(2):
                rows = cs["rows"][k]
                product = cube[it, 0, rows] + (x_ended[it, r, k] + x_chain[it, r, 2 + k])
                value = block[it, 0, rows]
                if it == 0:
                    f = factor[0:1, 0:1]
                    new = (1.5 * f) * value - (0.5 * f) * product
                else:
                    new = 1.5 * value - 0.5 * product
                if it == ITERS - 1:
                    o_ref[rows] = new
                else:
                    block[it + 1, 0, rows] = new

        sy, sz = {}, {}
        if it == 0:
            for k, peer in enumerate(y_peers, 1):
                sy[k] = copy(sums_y.at[0], sums_y.at[k], s_send.at[0], s_recv.at[0], peer)
            for k, peer in enumerate(z_peers, 1):
                sz[k] = copy(sums_z.at[0], sums_z.at[k], s_send.at[1], s_recv.at[1], peer)

        def sums1():
            tile = jnp.zeros((8, 128), F32)
            for v in (block[it, 0], panel[it, 1], panel[it, 2], panel[it, 3]):
                v = v.reshape(ROWS // 8, 8, STRIP)
                tile = tile + jnp.sum(v * v, axis=0)
            sums_y[0] = tile
            for made in sy.values():
                go(made)

        def sums2():
            all_here(sums_y.at[pl.ds(1, NY * NC - 1)], s_recv.at[0])
            sums_z[0] = jnp.sum(sums_y[...], axis=0)
            for made in sz.values():
                go(made)

        def sums3():
            all_here(sums_z.at[pl.ds(1, NZ - 1)], s_recv.at[1])
            total = jnp.sum(jnp.sum(sums_z[...], axis=0), keepdims=True)
            factor[...] = jnp.broadcast_to(jnp.sqrt(N / total), factor.shape)

        work = dict(
            own=own, zz=zz, put=put, xf=xf, xnear=xnear, xlast=xlast, mul=mul, s1=s1, s2=s2, s3=s3, s4=s4, s6=s6,
            rc=rc, rn=rn, re=re, fin=fin, sums1=sums1, sums2=sums2, sums3=sums3,
        )
        for name, *args in ORDER[it]:
            with jax.named_scope("_".join([f"i{it}", name, *map(str, args)])):
                work[name](*args)

    for it in range(ITERS):
        iteration(it)
    with jax.named_scope("sent"):
        slow = sum(LANES[s][1] * n for g, (_, n) in enumerate(GROUPS) for s in range(ns) if g * ns + s < THREE_STEPS)
        fast, slow = (NX * NZ - slow) // NX, slow // NX
        for it in range(ITERS):
            all_sent(block.at[it, pl.ds(0, NZ - 1)], z_send.at[it])
            all_sent(block.at[it, pl.ds(0, NX - 1)], x_send.at[it])
            all_sent(block.at[it, pl.ds(0, NX - 1)], r_send.at[it])
            all_sent(block.at[it], g_send.at[it, 0])
            all_sent(block.at[it, pl.ds(0, slow), pl.ds(0, HALF)], g_send.at[it, 1])
            all_sent(block.at[it, pl.ds(0, slow), pl.ds(0, PIECE)], g_send.at[it, 2])
            all_sent(block.at[it, pl.ds(0, fast)], g_send.at[it, 3])
        all_sent(sums_y.at[pl.ds(1, NY * NC - 1)], s_send.at[0])
        all_sent(sums_z.at[pl.ds(1, NZ - 1)], s_send.at[1])


def shards(matrix):
    dma = pltpu.SemaphoreType.DMA
    wide = NX * STRIP
    widths = [n * STRIP for _, n in LANES]

    def per_set(*shape):
        return [pltpu.VMEM((ITERS, NZ, *shape, width), F32) for width in widths]

    return pl.pallas_call(
        kernel,
        out_shape=pltpu.VMEM((ROWS, STRIP), F32),
        in_specs=[pl.BlockSpec(memory_space=pltpu.HBM)],
        out_specs=pl.BlockSpec(memory_space=pltpu.VMEM),
        scratch_shapes=[
            pltpu.VMEM((ITERS, NZ, ROWS, STRIP), F32),
            pltpu.VMEM((ITERS, NX, ROWS, STRIP), F32),
            pltpu.VMEM((ROWS, NZ * STRIP), BF),
            pltpu.VMEM((ROWS, NZ * STRIP), BF),
            pltpu.VMEM((ROWS, wide), BF),
            pltpu.VMEM((ROWS, wide), BF),
            pltpu.VMEM((NZ * STRIP, wide), BF),
            pltpu.VMEM((NZ * STRIP, wide), BF),
            *per_set(NC, SROWS),
            *per_set(SROWS),
            *per_set(SROWS),
            *per_set(SROWS),
            *per_set(SROWS),
            *per_set(SROWS),
            *per_set(NC, SROWS),
            pltpu.VMEM((ITERS, NX, ROWS, STRIP), F32),
            pltpu.VMEM((ITERS, 2, 4, PIECE, STRIP), F32),
            pltpu.VMEM((ITERS, 2, 2, PIECE, STRIP), F32),
            pltpu.VMEM((8, 128), F32),
            pltpu.VMEM((NY * NC, 8, 128), F32),
            pltpu.VMEM((NZ, 8, 128), F32),
            dma((ITERS,)),
            dma((ITERS, 3 * PIECES + 1)),
            dma((ITERS,)),
            dma((4,)),
            dma((ITERS,)),
            dma((2, 3)),
            dma((ITERS, 4)),
            dma((4 * len(GROUPS) * len(SETS),)),
            dma((2,)),
            dma((2,)),
            dma((2,)),
        ],
        compiler_params=pltpu.CompilerParams(
            collective_id=0, has_side_effects=True, vmem_limit_bytes=56 * 1024 * 1024
        ),
    )(matrix)


def solution(mesh):
    grid = Mesh(mesh.devices.reshape(NY, NC, NX, NZ), ("y", "c", "x", "z"))
    spec = P(("y", "c"), ("x", "z"))
    return jax.shard_map(shards, mesh=grid, in_specs=(spec,), out_specs=spec, check_vma=False)
```
